256 devices in a mesh: grid: 32 (over y, x, core), rows: 8 (over z).
Axes of the slice: x: 4, y: 4, z: 8, core: 2. Of those that a mesh axis runs over, the one named last changes fastest.
Arguments:
- density: bfloat16 [32, 128, 4096], P(None, 'rows', 'grid'), as said below
- basis_values: bfloat16 [64, 16, 128, 512], P('grid', None, 'rows'), may hold values from -0.59765625 to 0.59765625
- grid_points: float32 [64, 3, 512], P('grid'), may hold values from -4 to 4
- grid_weights: float32 [64, 512], P('grid'), may hold values from 0.05 to 1
- screened_blocks: int32 [64, 16], P('grid'), may hold values from 0 to 31, as said below
Outputs:
- exchange: float32 [32, 128, 4096], P(None, 'rows', 'grid')
The draws below stay inside these ranges and needn't reach their ends.
Inputs may be any that keep to these rules, and one draw needn't show every extreme that they name: density is symmetric: density[a, i, b * 128 + j] equals density[b, j, a * 128 + i]. `screened_blocks`: each row holds 16 distinct block numbers.
All inputs are finite; a program needn't handle non-finite values.
Results may differ from the reference program's by a relative error of at most 0.00055.
The reference program's roundings to bfloat16 on the way count: a program that leaves them out, or rounds other values in their place, can miss the bound.
Values may be sent and summed in bfloat16 or wider, within the bound.
A program may use at most 64 MiB of HBM per device.

```python
import math
import jax
import jax.numpy as jnp
from jax import lax

NBF = 4096
BS = 128
SIG = 16
PTS = 512
NBLK = 32
NBATCH = 64


def draw_density(key, part):
    key_off, key_diag = jax.random.split(jax.random.fold_in(key, 11), 2)
    noise = jax.random.normal(key_off, (NBF, NBF), jnp.float32) * (0.6 * (2.0 * NBF) ** (-0.5))
    dens = noise + noise.T
    diagonal = jax.random.uniform(key_diag, (NBF,), jnp.float32, 1.6, 2.6)
    dens = dens + jnp.diag(diagonal)
    return dens.reshape(NBF // BS, BS, NBF).astype(jnp.bfloat16)


def draw_screened_blocks(key, part):
    keys = jax.random.split(jax.random.fold_in(key, 7), NBATCH)
    picks = jax.vmap(lambda one_key: jax.random.permutation(one_key, NBF // BS)[:SIG])(keys)
    return picks.astype(jnp.int32)


def level_of(own_key, shape, cuts, least, largest):
    level = 1.0
    for position, shards_of in cuts:
        draws = jax.random.uniform(jax.random.fold_in(jax.random.fold_in(own_key, 6), position), (shards_of,), jnp.float32, least / len(cuts), largest / len(cuts))
        level = level * jnp.repeat(jnp.exp(draws), shape[position] // shards_of).reshape((-1,) + (1,) * (len(shape) - 1 - position))
    return level


def scatter_about(stream_key, extent, deviation, limit, cuts=(), dtype=jnp.bfloat16):
    values = deviation * jax.random.normal(stream_key, extent, jnp.float32)
    if cuts:
        values = values * level_of(stream_key, extent, cuts, -0.22, 0.18)
    return jnp.clip(values, -limit, limit).astype(dtype)


def setup_inputs(seed: int = 0) -> dict:
    key_of = jax.random.split(jax.random.key(seed), 6)
    return {
        "density": draw_density(jax.random.fold_in(key_of[5], 71), 0),
        "basis_values": scatter_about(key_of[1], (NBATCH, SIG, BS, PTS), 0.1, 0.59765625, ((0, 32), (2, 8))),
        "grid_points": jnp.clip(jax.random.uniform(key_of[2], (NBATCH, 3, PTS), jnp.float32, -4.0, 4.0) * level_of(key_of[2], (NBATCH, 3, PTS), ((0, 32),), -0.4, 0.0), -4.0, 4.0),
        "grid_weights": jnp.clip(jnp.exp(math.log(1.0) - 2.9957323 * jax.random.uniform(key_of[3], (NBATCH, PTS), jnp.float32) ** level_of(key_of[3], (NBATCH, PTS), ((0, 32),), -0.2, 0.2)), 0.05, 1.0),
        "screened_blocks": draw_screened_blocks(jax.random.fold_in(key_of[5], 71), 0),
    }


def reference(density, basis_values, grid_points, grid_weights, screened_blocks):
    dense = density.reshape(NBLK, BS, NBLK, BS)

    def one_batch(totals, items):
        values, places, weights, blocks = items
        chosen = dense[blocks][:, :, blocks, :].reshape(SIG * BS, SIG * BS)
        flat = values.reshape(SIG * BS, PTS)
        fmat = jnp.dot(chosen, flat, preferred_element_type=jnp.float32).astype(jnp.bfloat16)
        intersection = jnp.dot(flat.T, fmat, preferred_element_type=jnp.float32)
        diffs = places[:, :, None] - places[:, None, :]
        kern = 1.0 / jnp.sqrt(lax.optimization_barrier(jnp.sum(diffs * diffs, axis=0)) + 0.5)
        mixed = (weights[:, None] * kern * intersection).astype(jnp.bfloat16)
        potential = (jnp.dot(flat, mixed, preferred_element_type=jnp.float32) * weights[None, :]).astype(jnp.bfloat16)
        block_k = jnp.dot(flat, potential.T, preferred_element_type=jnp.float32).reshape(SIG, BS, SIG, BS)
        totals = totals.at[blocks[:, None], :, blocks[None, :], :].add(block_k.transpose(0, 2, 1, 3))
        return (totals, None)
    start_totals = jnp.zeros((NBLK, BS, NBLK, BS), jnp.float32)
    totals, unused = lax.scan(one_batch, start_totals, (basis_values, grid_points, grid_weights, screened_blocks))
    return totals.reshape(NBLK, BS, NBLK * BS)
```

```python
import jax
import jax.numpy as jnp
from jax import lax
from jax.experimental import pallas as pl
from jax.experimental.pallas import tpu as pltpu
from jax.sharding import PartitionSpec as P

MESH = pl.DeviceIdType.MESH
NX = 4
NY = 4
NZ = 8
NCHIP = NX * NY
BF16 = jnp.bfloat16
F32 = jnp.float32
NT = (((1,), (1,)), ((), ()))
TN = (((0,), (0,)), ((), ()))


def mod(a, n):
    return lax.rem(a, n)


def kernel(
    sel, inv, dens, xin, pts, wts, out,
    pg, xg, psel, fs, fr, mg, pot, xd, kc, kp, d0, s1, rb, cb, t1, rb2, cb2, z1, zr,
    x_s, x_r, p_s, p_r, q_s, q_r, f_s, f_r, m_s, m_r, d_s, d_r, a_s, a_r, b_s, b_r, z_s, z_r,
):
    g = lax.axis_index("grid")
    r = lax.axis_index("rows")
    core = mod(g, 2)
    chip = lax.div(g, 2)
    x = mod(chip, NX)
    y = lax.div(chip, NX)

    def at_plane(xx, yy):
        return (2 * (NX * yy + xx) + core, r)

    def at_z(rr):
        return (g, rr)

    partner = (2 * chip + 1 - core, r)

    def remote(src, dst, send, recv, device):
        return pltpu.make_async_remote_copy(
            src_ref=src, dst_ref=dst, send_sem=send, recv_sem=recv, device_id=device, device_id_type=MESH
        )

    bar = pltpu.get_barrier_semaphore()
    for k in range(1, NCHIP):
        device = at_plane(mod(x + k % NX, NX), mod(y + k // NX, NY))
        pl.semaphore_signal(bar, inc=1, device_id=device, device_id_type=MESH)
    for k in range(1, NZ):
        pl.semaphore_signal(bar, inc=1, device_id=at_z(mod(r + k, NZ)), device_id_type=MESH)
    pl.semaphore_signal(bar, inc=1, device_id=partner, device_id_type=MESH)
    pl.semaphore_wait(bar, NCHIP - 1 + NZ - 1 + 1)

    up, down = at_z(mod(r + 1, NZ)), at_z(mod(r + NZ - 1, NZ))

    def shard_of(d, t):
        return mod(r + (NZ - t if d == 0 else t), NZ)

    def x_copy(d, t, b):
        dst = xg.at[b, pl.ds(0, 16), shard_of(d, t)]
        src = xin.at[b] if t == 0 else dst
        return remote(src, dst, x_s.at[d, t, b], x_r.at[d, t, b], up if d == 0 else down)

    ring = [(d, t, b) for t in range(4) for b in range(2) for d in range(2) if t < 3 or b == d]

    def p_copy(k):
        device = at_plane(mod(x + mod(k, NX), NX), mod(y + lax.div(k, NX), NY))
        return remote(dens, pg.at[g], p_s.at[k], p_r.at[k], device)

    def p_forward(k):
        xs, ys = mod(x + NX - mod(k, NX), NX), mod(y + NY - lax.div(k, NX), NY)
        slot = 2 * (NX * ys + xs) + core
        src = dens if isinstance(k, int) else pg.at[slot]
        return remote(src, pg.at[slot], q_s.at[k], q_r.at[k], partner)

    for d, t, b in ring[:4]:
        x_copy(d, t, b).start()

    @pl.loop(1, NCHIP)
    def _(k):
        p_copy(k).start()

    pg[g] = dens[...]
    for b in range(2):
        xg[b, 0:16, r] = xin[b]
        xg[b, 16] = jnp.zeros(xg.shape[2:], BF16)
        kc[b, 16] = jnp.zeros(kc.shape[2:], F32)

    def x_step(t):
        for d, tt, b in ring:
            if tt == t:
                x_copy(d, t - 1, b).wait_recv()
                x_copy(d, t, b).start()

    x_step(1)
    x_step(2)

    p_forward(0).start()

    @pl.loop(1, NCHIP)
    def _(k):
        p_copy(k).wait_recv()
        p_forward(k).start()

    x_step(3)

    @pl.loop(0, NCHIP)
    def _(k):
        p_forward(k).wait_recv()

    @pl.loop(0, 16)
    def _(s):
        for b in range(2):
            row = sel[b, s]
            for c in range(16):
                psel[b, s, :, 128 * c : 128 * (c + 1)] = pg[sel[b, c], row]

    for d, t, b in ring:
        if t == 3 or (t == 2 and b != d):
            x_copy(d, t, b).wait_recv()

    for b in range(2):
        rows = psel[b].reshape(256, 2048)
        for h in range(2):
            f = jnp.dot(
                rows, xg[b, 0:16, :, :, 256 * h : 256 * (h + 1)].reshape(2048, 256), preferred_element_type=F32
            ).astype(BF16)
            fs[b, 2 * h] = f[:, 0:128].reshape(16, 16, 128)
            fs[b, 2 * h + 1] = f[:, 128:256].reshape(16, 16, 128)

    def f_copy(k):
        to = mod(r + k, NZ)
        return remote(fs.at[lax.div(to, 4), mod(to, 4)], fr.at[:, r], f_s.at[k], f_r.at[k], at_z(to))

    for k in (4, 3, 5, 2, 6, 1, 7):
        f_copy(k).start()
    my_b, my_q = lax.div(r, 4), mod(r, 4)
    fr[:, r] = fs[my_b, my_q]

    lanes = pl.ds(pl.multiple_of(128 * my_q, 128), 128)
    dist = jnp.zeros((128, 512), F32)
    for c in range(3):
        across = pts[my_b, c : c + 1, :]
        down_col = jnp.broadcast_to(pts[my_b, c : c + 1, lanes], (128, 128)).T
        diff = across - jnp.concatenate([down_col] * 4, axis=1)
        dist = dist + diff * diff
    scale = wts[my_b] * (1.0 / jnp.sqrt(dist + 0.5))

    for k in range(1, NZ):
        f_copy(k).wait_recv()
    inter = lax.dot_general(
        fr[...].reshape(2048, 128), xg[my_b, 0:16].reshape(2048, 512), TN, preferred_element_type=F32
    )
    mg[r] = (scale * inter).astype(BF16)

    def m_copy(d, t, h):
        ref = mg.at[shard_of(d, t), pl.ds(64 * h, 64)]
        return remote(ref, ref, m_s.at[d, t, h], m_r.at[d, t, h], up if d == 0 else down)

    for d, t, h in ring[:4]:
        m_copy(d, t, h).start()
    for d, t, h in ring[4:]:
        m_copy(d, t - 1, h).wait_recv()
        m_copy(d, t, h).start()
    for d, t, h in ring:
        if t == 3 or (t == 2 and h != d):
            m_copy(d, t, h).wait_recv()

    for b in range(2):
        m = mg[4 * b : 4 * b + 4].reshape(512, 512)
        full = lax.dot_general(xin[b].reshape(256, 512), m, NT, preferred_element_type=F32)
        pot[b] = (full * wts[b]).astype(BF16)

    def d_copy(rp):
        return remote(kp.at[1 - core, rp], d0.at[rp], d_s.at[rp], d_r.at[rp], partner)

    @pl.loop(0, 4)
    def _(p):
        for half in range(2):
            rp = p + 4 * half
            for b in range(2):
                for a in range(32):
                    xd[b, a] = xg[b, inv[b, a], rp]
                kc[b, 0:16] = lax.dot_general(
                    pot[b], xd[b].reshape(512, 512), NT, preferred_element_type=F32
                ).reshape(16, 16, 512)
            for v in range(4):
                for u in range(4):
                    for c in range(2):
                        nb = 2 * (NX * v + u if half == 0 else NX * u + v) + c
                        kp[c, rp, v, u] = kc[0, inv[0, nb]] + kc[1, inv[1, nb]]
            d_copy(rp).start()

    first = (x, y)
    second = (y, x)
    low, high = pl.ds(0, 8), pl.ds(8, 8)

    def along(half, stage, shift):
        if half == stage:
            return at_plane(mod(x + shift, NX), y)
        return at_plane(x, mod(y + shift, NY))

    def a_copy(half, rp, m):
        u = first[half]
        nxt, opp, prv = mod(u + 1, 4), mod(u + 2, 4), mod(u + 3, 4)
        src = (
            s1.at[rp, :, opp, low], s1.at[rp, :, nxt, high], cb.at[0, rp],
            s1.at[rp, :, opp, high], s1.at[rp, :, prv, low], cb.at[1, rp],
        )[m]
        return remote(src, rb.at[m, rp], a_s.at[m, rp], a_r.at[m, rp], along(half, 0, 1 if m < 3 else 3))

    def b_copy(half, rp, m):
        u = second[half]
        nxt, opp, prv = mod(u + 1, 4), mod(u + 2, 4), mod(u + 3, 4)
        src = (
            t1.at[rp, opp, low], t1.at[rp, nxt, high], cb2.at[0, rp],
            t1.at[rp, opp, high], t1.at[rp, prv, low], cb2.at[1, rp],
        )[m]
        return remote(src, rb2.at[m, rp], b_s.at[m, rp], b_r.at[m, rp], along(half, 1, 1 if m < 3 else 3))

    @pl.loop(0, 4)
    def _(p):
        for half in range(2):
            rp = p + 4 * half
            d_copy(rp).wait_recv()
            s1[rp] = kp[core, rp] + d0[rp]
            for m in (0, 3, 1, 4):
                a_copy(half, rp, m).start()

    @pl.loop(0, 4)
    def _(p):
        for half in range(2):
            rp = p + 4 * half
            u = first[half]
            a_copy(half, rp, 0).wait_recv()
            cb[0, rp] = rb[0, rp] + s1[rp, :, mod(u + 1, 4), 0:8]
            a_copy(half, rp, 2).start()
            a_copy(half, rp, 3).wait_recv()
            cb[1, rp] = rb[3, rp] + s1[rp, :, mod(u + 3, 4), 8:16]
            a_copy(half, rp, 5).start()

    @pl.loop(0, 4)
    def _(p):
        for half in range(2):
            rp = p + 4 * half
            u = first[half]
            for m in (1, 4, 2, 5):
                a_copy(half, rp, m).wait_recv()
            t1[rp, :, 0:8] = s1[rp, :, u, 0:8] + rb[4, rp] + rb[2, rp]
            t1[rp, :, 8:16] = s1[rp, :, u, 8:16] + rb[1, rp] + rb[5, rp]
            for m in (0, 3, 1, 4):
                b_copy(half, rp, m).start()

    @pl.loop(0, 4)
    def _(p):
        for half in range(2):
            rp = p + 4 * half
            u = second[half]
            b_copy(half, rp, 0).wait_recv()
            cb2[0, rp] = rb2[0, rp] + t1[rp, mod(u + 1, 4), 0:8]
            b_copy(half, rp, 2).start()
            b_copy(half, rp, 3).wait_recv()
            cb2[1, rp] = rb2[3, rp] + t1[rp, mod(u + 3, 4), 8:16]
            b_copy(half, rp, 5).start()

    def z_copy(rp):
        return remote(z1.at[rp], zr.at[r], z_s.at[rp], z_r.at[r], at_z(rp))

    @pl.loop(0, 4)
    def _(p):
        for half in range(2):
            rp = p + 4 * half
            u = second[half]
            for m in (1, 4, 2, 5):
                b_copy(half, rp, m).wait_recv()
            z1[rp, 0:8] = t1[rp, u, 0:8] + rb2[4, rp] + rb2[2, rp]
            z1[rp, 8:16] = t1[rp, u, 8:16] + rb2[1, rp] + rb2[5, rp]

            @pl.when(rp != r)
            def _():
                z_copy(rp).start()

    zr[r] = z1[r]

    @pl.loop(1, NZ)
    def _(k):
        source = mod(r + k, NZ)
        remote(z1.at[source], zr.at[source], z_s.at[source], z_r.at[source], at_z(source)).wait_recv()

    for c in range(4):
        block = zr[:, :, 128 * c : 128 * (c + 1)].reshape(128, 128)
        out[8 * c : 8 * c + 8] = block.T.reshape(8, 16, 128)

    for d, t, b in ring:
        x_copy(d, t, b).wait_send()
        m_copy(d, t, b).wait_send()

    p_forward(0).wait_send()

    @pl.loop(1, NCHIP)
    def _(k):
        p_copy(k).wait_send()
        p_forward(k).wait_send()

    @pl.loop(1, NZ)
    def _(k):
        f_copy(k).wait_send()
        z_copy(mod(r + k, NZ)).wait_send()

    @pl.loop(0, 4)
    def _(p):
        for half in range(2):
            rp = p + 4 * half
            d_copy(rp).wait_send()
            for m in range(6):
                a_copy(half, rp, m).wait_send()
                b_copy(half, rp, m).wait_send()


def body(density, basis_values, grid_points, grid_weights, screened_blocks):
    wanted = jnp.arange(32, dtype=jnp.int32)
    hits = screened_blocks[:, :, None] == wanted[None, None, :]
    inverse = jnp.min(jnp.where(hits, jnp.arange(16, dtype=jnp.int32)[None, :, None], 16), axis=1)
    vmem = pl.BlockSpec(memory_space=pltpu.VMEM)
    smem = pl.BlockSpec(memory_space=pltpu.SMEM)
    dma = pltpu.SemaphoreType.DMA
    return pl.pallas_call(
        kernel,
        out_shape=jax.ShapeDtypeStruct((32, 16, 128), F32),
        in_specs=[smem, smem, vmem, vmem, vmem, vmem],
        out_specs=vmem,
        scratch_shapes=[
            pltpu.VMEM((32, 32, 16, 128), BF16),
            pltpu.VMEM((2, 17, 8, 16, 512), BF16),
            pltpu.VMEM((2, 16, 16, 2048), BF16),
            pltpu.VMEM((2, 4, 16, 16, 128), BF16),
            pltpu.VMEM((16, 8, 16, 128), BF16),
            pltpu.VMEM((8, 128, 512), BF16),
            pltpu.VMEM((2, 256, 512), BF16),
            pltpu.VMEM((2, 32, 16, 512), BF16),
            pltpu.VMEM((2, 17, 16, 512), F32),
            pltpu.VMEM((2, 8, 4, 4, 16, 512), F32),
            pltpu.VMEM((8, 4, 4, 16, 512), F32),
            pltpu.VMEM((8, 4, 4, 16, 512), F32),
            pltpu.VMEM((6, 8, 4, 8, 512), F32),
            pltpu.VMEM((2, 8, 4, 8, 512), F32),
            pltpu.VMEM((8, 4, 16, 512), F32),
            pltpu.VMEM((6, 8, 8, 512), F32),
            pltpu.VMEM((2, 8, 8, 512), F32),
            pltpu.VMEM((8, 16, 512), F32),
            pltpu.VMEM((8, 16, 512), F32),
            dma((2, 4, 2)), dma((2, 4, 2)),
            dma((16,)), dma((16,)),
            dma((16,)), dma((16,)),
            dma((8,)), dma((8,)),
            dma((2, 4, 2)), dma((2, 4, 2)),
            dma((8,)), dma((8,)),
            dma((6, 8)), dma((6, 8)),
            dma((6, 8)), dma((6, 8)),
            dma((8,)), dma((8,)),
        ],
        compiler_params=pltpu.CompilerParams(
            collective_id=0, has_side_effects=True, vmem_limit_bytes=60 * 1024 * 1024
        ),
        cost_estimate=pl.CostEstimate(flops=4_000_000_000, bytes_accessed=2_000_000, transcendentals=100_000),
        name="exchange",
    )(screened_blocks, inverse, density, basis_values, grid_points, grid_weights[:, None, :])


def solution(mesh):
    placed = (
        P(None, "rows", "grid"),
        P("grid", None, "rows", None),
        P("grid", None, None),
        P("grid", None),
        P("grid", None),
    )
    return jax.shard_map(
        body, mesh=mesh, in_specs=placed, out_specs=P(None, "rows", "grid"), check_vma=False
    )
```

```python
import jax
import jax.numpy as jnp
from jax import lax
from jax.experimental import pallas as pl
from jax.experimental.pallas import tpu as pltpu
from jax.sharding import PartitionSpec as P

MESH = pl.DeviceIdType.MESH
NX = 4
NY = 4
NZ = 8
BF16 = jnp.bfloat16
F32 = jnp.float32
NT = (((1,), (1,)), ((), ()))
FAR_FIRST = (4, 3, 5, 2, 6, 1, 7)


def mod(a, n):
    return lax.rem(a, n)


def kernel(
    sel, dens, xin, pts, wts, out,
    inv, pg, xg, psel, tcol, scale, wcol, fs, fr, ps, pr, pot, xd, kc, kp, d0, s1, rb, cb, t1, rb2, cb2, z1, zr,
    x_s, x_r, p_s, p_r, q_s, q_r, f_s, f_r, m_s, m_r, d_s, d_r, a_s, a_r, b_s, b_r, z_s, z_r,
):
    g = lax.axis_index("grid")
    r = lax.axis_index("rows")
    core = mod(g, 2)
    chip = lax.div(g, 2)
    x = mod(chip, NX)
    y = lax.div(chip, NX)
    finish = []

    def at_plane(xx, yy):
        return (2 * (NX * yy + xx) + core, r)

    def at_z(rr):
        return (g, rr)

    partner = (2 * chip + 1 - core, r)
    up, down = at_z(mod(r + 1, NZ)), at_z(mod(r + NZ - 1, NZ))
    east, west = at_plane(mod(x + 1, NX), y), at_plane(mod(x + NX - 1, NX), y)
    north, south = at_plane(x, mod(y + 1, NY)), at_plane(x, mod(y + NY - 1, NY))

    def remote(src, dst, send, recv, device):
        return pltpu.make_async_remote_copy(
            src_ref=src, dst_ref=dst, send_sem=send, recv_sem=recv, device_id=device, device_id_type=MESH
        )

    bar = pltpu.get_barrier_semaphore()
    for device in (up, down, east, west, north, south, partner):
        pl.semaphore_signal(bar, inc=1, device_id=device, device_id_type=MESH)
    pl.semaphore_wait(bar, 7)

    def x_copy(d, t, b):
        shard = mod(r + (NZ - t if d == 0 else t), NZ)
        part = pl.ds(0, 16) if t < 3 else pl.ds(8 * d, 8)
        dst = xg.at[b, part, shard]
        src = xin.at[b] if t == 0 else dst
        return remote(src, dst, x_s.at[d, t, b], x_r.at[d, t, b], up if d == 0 else down)

    def x_send(t, b):
        for d in range(2):
            if t > 0:
                x_copy(d, t - 1, b).wait_recv()
            x_copy(d, t, b).start()

    def px_copy(d, t):
        if t == 0:
            src, dst = dens, pg.at[y, x, core]
        else:
            dst = pg.at[y, mod(x + (3 if d == 0 else 1), NX), core, pl.ds(16 * d, 16)]
            src = dst
        return remote(src, dst, p_s.at[0, d, t], p_r.at[0, d, t], east if d == 0 else west)

    def py_copy(d, t):
        if t == 0:
            ref = pg.at[y, :, core]
        else:
            ref = pg.at[mod(y + (3 if d == 0 else 1), NY), :, core, pl.ds(16 * d, 16)]
        return remote(ref, ref, p_s.at[1, d, t], p_r.at[1, d, t], north if d == 0 else south)

    def pq_copy(k):
        ref = pg.at[mod(y + k, NY), :, core]
        return remote(ref, ref, q_s.at[k], q_r.at[k], partner)

    x_send(0, 0)
    px_copy(0, 0).start()
    px_copy(1, 0).start()
    x_send(0, 1)

    pg[y, x, core] = dens[...]
    for b in range(2):
        xg[b, 0:16, r] = xin[b]
        xg[b, 16] = jnp.zeros(xg.shape[2:], BF16)
        kc[b, 16] = jnp.zeros(kc.shape[2:], F32)

    px_copy(0, 0).wait_recv()
    px_copy(0, 1).start()
    px_copy(1, 0).wait_recv()
    px_copy(1, 1).start()

    @pl.loop(0, 32)
    def _(nb):
        for b in range(2):
            at = jnp.int32(16)
            for s in range(16):
                at = jnp.where(sel[b, s] == nb, s, at)
            inv[b, nb] = at

    x_send(1, 0)

    px_copy(0, 1).wait_recv()
    px_copy(1, 1).wait_recv()
    py_copy(0, 0).start()
    py_copy(1, 0).start()
    pq_copy(0).start()

    lanes = pl.ds(pl.multiple_of(128 * lax.div(r, 2), 128), 128)
    mine = pl.ds(pl.multiple_of(64 * mod(r, 2), 64), 64)
    for b in range(2):
        for c in range(4):
            row = pts[c, b : b + 1, lanes] if c < 3 else wts[b : b + 1, lanes]
            tcol[b, c] = jnp.broadcast_to(row, (128, 128)).T
        dist = jnp.zeros((64, 512), F32)
        for c in range(3):
            diff = pts[c, b : b + 1, :] - jnp.concatenate([tcol[b, c, mine]] * 4, axis=1)
            dist = dist + diff * diff
        scale[b] = wts[b : b + 1, :] * (1.0 / jnp.sqrt(dist + 0.5))
        wcol[b] = tcol[b, 3, mine]

    x_send(1, 1)
    x_send(2, 0)

    for d in range(2):
        py_copy(d, 0).wait_recv()
        py_copy(d, 1).start()
    pq_copy(1).start()
    pq_copy(3).start()

    x_send(2, 1)
    x_send(3, 0)

    py_copy(0, 1).wait_recv()
    py_copy(1, 1).wait_recv()
    pq_copy(2).start()

    x_send(3, 1)

    for k in range(4):
        pq_copy(k).wait_recv()

    def finish_gathers():
        for d in range(2):
            for t in range(4):
                for b in range(2):
                    x_copy(d, t, b).wait_send()
            for t in range(2):
                px_copy(d, t).wait_send()
                py_copy(d, t).wait_send()
        for k in range(4):
            pq_copy(k).wait_send()

    finish.append(finish_gathers)

    @pl.loop(0, 16)
    def _(s):
        for b in range(2):
            row = sel[b, s]
            for c in range(16):
                col = sel[b, c]
                psel[b, s, :, 128 * c : 128 * (c + 1)] = pg[
                    lax.div(col, 8), mod(lax.div(col, 2), 4), mod(col, 2), row
                ]

    def f_copy(b, k):
        to = mod(r + k, NZ)
        return remote(fs.at[b, to], fr.at[b, r], f_s.at[b, k], f_r.at[b, k], at_z(to))

    for b in range(2):
        for d in range(2):
            x_copy(d, 3, b).wait_recv()
        f = jnp.dot(
            psel[b].reshape(256, 2048), xg[b, 0:16].reshape(2048, 512), preferred_element_type=F32
        ).astype(BF16)
        fs[b] = f.T.reshape(8, 64, 256)
        for k in FAR_FIRST:
            f_copy(b, k).start()
        fr[b, r] = fs[b, r]

    def finish_f():
        for b in range(2):
            for k in FAR_FIRST:
                f_copy(b, k).wait_send()

    finish.append(finish_f)

    def m_copy(b, k):
        to = mod(r + k, NZ)
        return remote(ps.at[b, to], pr.at[b, r], m_s.at[b, k], m_r.at[b, k], at_z(to))

    for b in range(2):
        for k in FAR_FIRST:
            f_copy(b, k).wait_recv()
        inter = jnp.zeros((64, 512), F32)
        for s in range(8):
            inter = inter + jnp.dot(fr[b, s], xg[b, 0:16, s].reshape(256, 512), preferred_element_type=F32)
        mixed = (scale[b] * inter).astype(BF16)
        factor = jnp.concatenate([wcol[b]] * 2, axis=1)
        for s in range(8):
            p = lax.dot_general(mixed, xg[b, 0:16, s].reshape(256, 512), NT, preferred_element_type=F32)
            ps[b, s] = (p * factor).astype(BF16)
        for k in FAR_FIRST:
            m_copy(b, k).start()
        pr[b, r] = ps[b, r]

    def finish_m():
        for b in range(2):
            for k in FAR_FIRST:
                m_copy(b, k).wait_send()

    finish.append(finish_m)

    for b in range(2):
        for k in FAR_FIRST:
            m_copy(b, k).wait_recv()
        pot[b] = pr[b].reshape(512, 256).T

    first = (x, y)
    second = (y, x)
    low, high = pl.ds(0, 8), pl.ds(8, 8)

    def d_copy(rp):
        return remote(kp.at[1 - core, rp], d0.at[rp], d_s.at[rp], d_r.at[rp], partner)

    def along(half, stage, shift):
        if half == stage:
            return at_plane(mod(x + shift, NX), y)
        return at_plane(x, mod(y + shift, NY))

    def a_copy(half, rp, m):
        u = first[half]
        nxt, opp, prv = mod(u + 1, 4), mod(u + 2, 4), mod(u + 3, 4)
        src = (
            s1.at[rp, :, opp, low], s1.at[rp, :, nxt, high], cb.at[0, rp],
            s1.at[rp, :, opp, high], s1.at[rp, :, prv, low], cb.at[1, rp],
        )[m]
        return remote(src, rb.at[m, rp], a_s.at[m, rp], a_r.at[m, rp], along(half, 0, 1 if m < 3 else 3))

    def b_copy(half, rp, m):
        u = second[half]
        nxt, opp, prv = mod(u + 1, 4), mod(u + 2, 4), mod(u + 3, 4)
        src = (
            t1.at[rp, opp, low], t1.at[rp, nxt, high], cb2.at[0, rp],
            t1.at[rp, opp, high], t1.at[rp, prv, low], cb2.at[1, rp],
        )[m]
        return remote(src, rb2.at[m, rp], b_s.at[m, rp], b_r.at[m, rp], along(half, 1, 1 if m < 3 else 3))

    def make_slice(half, rp):
        for b in range(2):
            for a in range(32):
                xd[b, a] = xg[b, inv[b, a], rp]
            kc[b, 0:16] = lax.dot_general(
                pot[b], xd[b].reshape(512, 512), NT, preferred_element_type=F32
            ).reshape(16, 16, 512)
        for v in range(4):
            for u in range(4):
                for c in range(2):
                    nb = 2 * (NX * v + u if half == 0 else NX * u + v) + c
                    kp[c, rp, v, u] = kc[0, inv[0, nb]] + kc[1, inv[1, nb]]
        d_copy(rp).start()

    def send_slice(half, rp):
        d_copy(rp).wait_recv()
        s1[rp] = kp[core, rp] + d0[rp]
        for m in (0, 3, 1, 4):
            a_copy(half, rp, m).start()

    def finish_a():
        @pl.loop(0, 4)
        def _(p):
            for half in range(2):
                d_copy(p + 4 * half).wait_send()
                for m in range(6):
                    a_copy(half, p + 4 * half, m).wait_send()

    finish.append(finish_a)

    @pl.loop(0, 4)
    def _(p):
        for half in range(2):
            make_slice(half, p + 4 * half)

            @pl.when(p > 0)
            def _():
                send_slice(half, p + 4 * half - 1)

    for half in range(2):
        send_slice(half, 3 + 4 * half)


    @pl.loop(0, 4)
    def _(p):
        for half in range(2):
            rp = p + 4 * half
            u = first[half]
            a_copy(half, rp, 0).wait_recv()
            cb[0, rp] = rb[0, rp] + s1[rp, :, mod(u + 1, 4), 0:8]
            a_copy(half, rp, 2).start()
            a_copy(half, rp, 3).wait_recv()
            cb[1, rp] = rb[3, rp] + s1[rp, :, mod(u + 3, 4), 8:16]
            a_copy(half, rp, 5).start()

    @pl.loop(0, 4)
    def _(p):
        for half in range(2):
            rp = p + 4 * half
            u = first[half]
            for m in (1, 4, 2, 5):
                a_copy(half, rp, m).wait_recv()
            t1[rp, :, 0:8] = s1[rp, :, u, 0:8] + rb[4, rp] + rb[2, rp]
            t1[rp, :, 8:16] = s1[rp, :, u, 8:16] + rb[1, rp] + rb[5, rp]
            for m in (0, 3, 1, 4):
                b_copy(half, rp, m).start()

    @pl.loop(0, 4)
    def _(p):
        for half in range(2):
            rp = p + 4 * half
            u = second[half]
            b_copy(half, rp, 0).wait_recv()
            cb2[0, rp] = rb2[0, rp] + t1[rp, mod(u + 1, 4), 0:8]
            b_copy(half, rp, 2).start()
            b_copy(half, rp, 3).wait_recv()
            cb2[1, rp] = rb2[3, rp] + t1[rp, mod(u + 3, 4), 8:16]
            b_copy(half, rp, 5).start()

    def z_copy(rp):
        return remote(z1.at[rp], zr.at[r], z_s.at[rp], z_r.at[r], at_z(rp))

    @pl.loop(0, 4)
    def _(p):
        for half in range(2):
            rp = p + 4 * half
            u = second[half]
            for m in (1, 4, 2, 5):
                b_copy(half, rp, m).wait_recv()
            z1[rp, 0:8] = t1[rp, u, 0:8] + rb2[4, rp] + rb2[2, rp]
            z1[rp, 8:16] = t1[rp, u, 8:16] + rb2[1, rp] + rb2[5, rp]

            @pl.when(rp != r)
            def _():
                z_copy(rp).start()

    zr[r] = z1[r]

    @pl.loop(1, NZ)
    def _(k):
        source = mod(r + k, NZ)
        remote(z1.at[source], zr.at[source], z_s.at[source], z_r.at[source], at_z(source)).wait_recv()

    for c in range(4):
        block = zr[:, :, 128 * c : 128 * (c + 1)].reshape(128, 128)
        out[8 * c : 8 * c + 8] = block.T.reshape(8, 16, 128)

    for waits in finish:
        waits()

    @pl.loop(0, 4)
    def _(p):
        for half in range(2):
            for m in range(6):
                b_copy(half, p + 4 * half, m).wait_send()

    @pl.loop(1, NZ)
    def _(k):
        z_copy(mod(r + k, NZ)).wait_send()


def body(density, basis_values, grid_points, grid_weights, screened_blocks):
    vmem = pl.BlockSpec(memory_space=pltpu.VMEM)
    smem = pl.BlockSpec(memory_space=pltpu.SMEM)
    dma = pltpu.SemaphoreType.DMA
    return pl.pallas_call(
        kernel,
        out_shape=jax.ShapeDtypeStruct((32, 16, 128), F32),
        in_specs=[smem, vmem, vmem, vmem, vmem],
        out_specs=vmem,
        scratch_shapes=[
            pltpu.SMEM((2, 32), jnp.int32),
            pltpu.VMEM((4, 4, 2, 32, 16, 128), BF16),
            pltpu.VMEM((2, 17, 8, 16, 512), BF16),
            pltpu.VMEM((2, 16, 16, 2048), BF16),
            pltpu.VMEM((2, 4, 128, 128), F32),
            pltpu.VMEM((2, 64, 512), F32),
            pltpu.VMEM((2, 64, 128), F32),
            pltpu.VMEM((2, 8, 64, 256), BF16),
            pltpu.VMEM((2, 8, 64, 256), BF16),
            pltpu.VMEM((2, 8, 64, 256), BF16),
            pltpu.VMEM((2, 8, 64, 256), BF16),
            pltpu.VMEM((2, 256, 512), BF16),
            pltpu.VMEM((2, 32, 16, 512), BF16),
            pltpu.VMEM((2, 17, 16, 512), F32),
            pltpu.VMEM((2, 8, 4, 4, 16, 512), F32),
            pltpu.VMEM((8, 4, 4, 16, 512), F32),
            pltpu.VMEM((8, 4, 4, 16, 512), F32),
            pltpu.VMEM((6, 8, 4, 8, 512), F32),
            pltpu.VMEM((2, 8, 4, 8, 512), F32),
            pltpu.VMEM((8, 4, 16, 512), F32),
            pltpu.VMEM((6, 8, 8, 512), F32),
            pltpu.VMEM((2, 8, 8, 512), F32),
            pltpu.VMEM((8, 16, 512), F32),
            pltpu.VMEM((8, 16, 512), F32),
            dma((2, 4, 2)), dma((2, 4, 2)),
            dma((2, 2, 2)), dma((2, 2, 2)),
            dma((4,)), dma((4,)),
            dma((2, 8)), dma((2, 8)),
            dma((2, 8)), dma((2, 8)),
            dma((8,)), dma((8,)),
            dma((6, 8)), dma((6, 8)),
            dma((6, 8)), dma((6, 8)),
            dma((8,)), dma((8,)),
        ],
        compiler_params=pltpu.CompilerParams(
            collective_id=0, has_side_effects=True, vmem_limit_bytes=60 * 1024 * 1024
        ),
        cost_estimate=pl.CostEstimate(flops=4_000_000_000, bytes_accessed=2_000_000, transcendentals=100_000),
        name="exchange",
    )(screened_blocks, density, basis_values, jnp.transpose(grid_points, (1, 0, 2)), grid_weights)


def solution(mesh):
    placed = (
        P(None, "rows", "grid"),
        P("grid", None, "rows", None),
        P("grid", None, None),
        P("grid", None),
        P("grid", None),
    )
    return jax.shard_map(
        body, mesh=mesh, in_specs=placed, out_specs=P(None, "rows", "grid"), check_vma=False
    )
```

```python
import jax
import jax.numpy as jnp
from jax import lax
from jax.experimental import pallas as pl
from jax.experimental.pallas import tpu as pltpu
from jax.sharding import PartitionSpec as P

MESH = pl.DeviceIdType.MESH
NX = 4
NY = 4
NZ = 8
BF16 = jnp.bfloat16
F32 = jnp.float32
NT = (((1,), (1,)), ((), ()))
FAR_FIRST = (4, 3, 5, 2, 6, 1, 7)


def mod(a, n):
    return lax.rem(a, n)


def kernel(
    sel, dens, xin, pts, wts, out,
    inv, pg, xg, psel, tcol, scale, wcol, fs, fr, ps, pr, pot, xd, k0, k1, kp, d0, s1, rb, cb, t1, rb2, z1,
    o_s, x_s, x_r, p_s, p_r, q_s, q_r, f_s, f_r, m_s, m_r, d_s, d_r, a_s, a_r, b_s, b_r, z_s, z_r,
):
    g = lax.axis_index("grid")
    r = lax.axis_index("rows")
    core = mod(g, 2)
    chip = lax.div(g, 2)
    x = mod(chip, NX)
    y = lax.div(chip, NX)
    finish = []

    def at_plane(xx, yy):
        return (2 * (NX * yy + xx) + core, r)

    def at_z(rr):
        return (g, rr)

    partner = (2 * chip + 1 - core, r)
    up, down = at_z(mod(r + 1, NZ)), at_z(mod(r + NZ - 1, NZ))
    east, west = at_plane(mod(x + 1, NX), y), at_plane(mod(x + NX - 1, NX), y)
    north, south = at_plane(x, mod(y + 1, NY)), at_plane(x, mod(y + NY - 1, NY))

    def remote(src, dst, send, recv, device):
        return pltpu.make_async_remote_copy(
            src_ref=src, dst_ref=dst, send_sem=send, recv_sem=recv, device_id=device, device_id_type=MESH
        )

    own = [pltpu.make_async_copy(xin.at[b], xg.at[b, pl.ds(0, 16), r], o_s.at[b]) for b in range(2)]
    own.append(pltpu.make_async_copy(dens, pg.at[y, x, core], o_s.at[2]))
    for copy in own:
        copy.start()
    bar = pltpu.get_barrier_semaphore()
    for device in (up, down, east, west, north, south, partner):
        pl.semaphore_signal(bar, inc=1, device_id=device, device_id_type=MESH)
    pl.semaphore_wait(bar, 7)
    own[0].wait()

    def x_copy(d, t, b):
        shard = mod(r + (NZ - t if d == 0 else t), NZ)
        part = pl.ds(0, 16) if t < 3 else pl.ds(8 * d, 8)
        dst = xg.at[b, part, shard]
        return remote(dst, dst, x_s.at[d, t, b], x_r.at[d, t, b], up if d == 0 else down)

    def x_send(t, b):
        for d in range(2):
            if t > 0:
                x_copy(d, t - 1, b).wait_recv()
            x_copy(d, t, b).start()

    def px_copy(d, t):
        if t == 0:
            ref = pg.at[y, x, core]
        else:
            ref = pg.at[y, mod(x + (3 if d == 0 else 1), NX), core, pl.ds(16 * d, 16)]
        return remote(ref, ref, p_s.at[0, d, t], p_r.at[0, d, t], east if d == 0 else west)

    def py_copy(d, t):
        if t == 0:
            ref = pg.at[y, :, core]
        else:
            ref = pg.at[mod(y + (3 if d == 0 else 1), NY), :, core, pl.ds(16 * d, 16)]
        return remote(ref, ref, p_s.at[1, d, t], p_r.at[1, d, t], north if d == 0 else south)

    def pq_copy(k):
        ref = pg.at[mod(y + k, NY), :, core]
        return remote(ref, ref, q_s.at[k], q_r.at[k], partner)

    x_send(0, 0)
    own[2].wait()
    px_copy(0, 0).start()
    px_copy(1, 0).start()
    own[1].wait()
    x_send(0, 1)

    for rp in range(8):
        k0[rp, 16] = jnp.zeros(k0.shape[2:], F32)
    for half in range(2):
        k1[half, 16] = jnp.zeros(k1.shape[2:], F32)
    for b in range(2):
        xg[b, 16] = jnp.zeros(xg.shape[2:], BF16)

    px_copy(0, 0).wait_recv()
    px_copy(0, 1).start()
    px_copy(1, 0).wait_recv()
    px_copy(1, 1).start()

    @pl.loop(0, 32)
    def _(nb):
        for b in range(2):
            at = jnp.int32(16)
            for s in range(16):
                at = jnp.where(sel[b, s] == nb, s, at)
            inv[b, nb] = at

    x_send(1, 0)

    px_copy(0, 1).wait_recv()
    px_copy(1, 1).wait_recv()
    py_copy(0, 0).start()
    py_copy(1, 0).start()
    pq_copy(0).start()

    lanes = pl.ds(pl.multiple_of(128 * lax.div(r, 2), 128), 128)
    mine = pl.ds(pl.multiple_of(64 * mod(r, 2), 64), 64)
    for b in range(2):
        for c in range(4):
            row = pts[c, b : b + 1, lanes] if c < 3 else wts[b : b + 1, lanes]
            tcol[b, c] = jnp.broadcast_to(row, (128, 128)).T
        dist = jnp.zeros((64, 512), F32)
        for c in range(3):
            diff = pts[c, b : b + 1, :] - jnp.concatenate([tcol[b, c, mine]] * 4, axis=1)
            dist = dist + diff * diff
        scale[b] = wts[b : b + 1, :] * (1.0 / jnp.sqrt(dist + 0.5))
        wcol[b] = tcol[b, 3, mine]

    x_send(1, 1)
    x_send(2, 0)

    for d in range(2):
        py_copy(d, 0).wait_recv()
        py_copy(d, 1).start()
    pq_copy(1).start()
    pq_copy(3).start()

    x_send(2, 1)
    x_send(3, 0)

    py_copy(0, 1).wait_recv()
    py_copy(1, 1).wait_recv()
    pq_copy(2).start()

    x_send(3, 1)

    for k in range(4):
        pq_copy(k).wait_recv()

    def finish_gathers():
        for d in range(2):
            for t in range(4):
                for b in range(2):
                    x_copy(d, t, b).wait_send()
            for t in range(2):
                px_copy(d, t).wait_send()
                py_copy(d, t).wait_send()
        for k in range(4):
            pq_copy(k).wait_send()

    finish.append(finish_gathers)

    @pl.loop(0, 16)
    def _(s):
        for b in range(2):
            row = sel[b, s]
            for c in range(16):
                col = sel[b, c]
                psel[b, s, :, 128 * c : 128 * (c + 1)] = pg[
                    lax.div(col, 8), mod(lax.div(col, 2), 4), mod(col, 2), row
                ]

    def f_copy(b, k):
        to = mod(r + k, NZ)
        return remote(fs.at[b, to], fr.at[b, r], f_s.at[b, k], f_r.at[b, k], at_z(to))

    for b in range(2):
        for d in range(2):
            x_copy(d, 3, b).wait_recv()
        f = jnp.dot(
            psel[b].reshape(256, 2048), xg[b, 0:16].reshape(2048, 512), preferred_element_type=F32
        ).astype(BF16)
        fs[b] = f.T.reshape(8, 64, 256)
        for k in FAR_FIRST:
            f_copy(b, k).start()
        fr[b, r] = fs[b, r]

    def finish_f():
        for b in range(2):
            for k in FAR_FIRST:
                f_copy(b, k).wait_send()

    finish.append(finish_f)

    def m_copy(b, k):
        to = mod(r + k, NZ)
        return remote(ps.at[b, to], pr.at[b, r], m_s.at[b, k], m_r.at[b, k], at_z(to))

    for b in range(2):
        for k in FAR_FIRST:
            f_copy(b, k).wait_recv()
        inter = jnp.zeros((64, 512), F32)
        for s in range(8):
            inter = inter + jnp.dot(fr[b, s], xg[b, 0:16, s].reshape(256, 512), preferred_element_type=F32)
        mixed = (scale[b] * inter).astype(BF16)
        factor = jnp.concatenate([wcol[b]] * 2, axis=1)
        for s in range(8):
            p = lax.dot_general(mixed, xg[b, 0:16, s].reshape(256, 512), NT, preferred_element_type=F32)
            ps[b, s] = (p * factor).astype(BF16)
        for k in FAR_FIRST:
            m_copy(b, k).start()
        pr[b, r] = ps[b, r]

    def finish_m():
        for b in range(2):
            for k in FAR_FIRST:
                m_copy(b, k).wait_send()

    finish.append(finish_m)

    def potential(b):
        for k in FAR_FIRST:
            m_copy(b, k).wait_recv()
        pot[b] = pr[b].reshape(512, 256).T

    potential(0)

    @pl.loop(0, 8)
    def _(rp):
        for a in range(32):
            xd[8, a] = xg[0, inv[0, a], rp]
        k0[rp, 0:16] = lax.dot_general(
            pot[0], xd[8].reshape(512, 512), NT, preferred_element_type=F32
        ).reshape(16, 16, 512)
        for a in range(32):
            xd[rp, a] = xg[1, inv[1, a], rp]

    potential(1)

    first = (x, y)
    second = (y, x)
    low, high = pl.ds(0, 8), pl.ds(8, 8)

    def d_copy(rp):
        return remote(kp.at[rp], d0.at[rp], d_s.at[rp], d_r.at[rp], partner)

    def along(half, stage, shift):
        if half == stage:
            return at_plane(mod(x + shift, NX), y)
        return at_plane(x, mod(y + shift, NY))

    def a_copy(half, rp, m):
        u = first[half]
        nxt, opp, prv = mod(u + 1, 4), mod(u + 2, 4), mod(u + 3, 4)
        src = (
            s1.at[rp, :, opp, low], s1.at[rp, :, nxt, high], cb.at[0, rp],
            s1.at[rp, :, opp, high], s1.at[rp, :, prv, low], cb.at[1, rp],
        )[m]
        return remote(src, rb.at[m, rp], a_s.at[m, rp], a_r.at[m, rp], along(half, 0, 1 if m < 3 else 3))

    def b_copy(half, rp, m):
        shift = (2, 1, 3)[m]
        src = t1.at[rp, mod(second[half] + shift, 4)]
        return remote(src, rb2.at[m, rp], b_s.at[m, rp], b_r.at[m, rp], along(half, 1, shift))

    def make_slice(half, rp):
        k1[half, 0:16] = lax.dot_general(
            pot[1], xd[rp].reshape(512, 512), NT, preferred_element_type=F32
        ).reshape(16, 16, 512)
        for ref, c in ((kp, 1 - core), (s1, core)):
            for v in range(4):
                for u in range(4):
                    nb = 2 * (NX * v + u if half == 0 else NX * u + v) + c
                    ref[rp, v, u] = k0[rp, inv[0, nb]] + k1[half, inv[1, nb]]
            if ref is kp:
                d_copy(rp).start()

    def send_slice(half, rp):
        d_copy(rp).wait_recv()
        s1[rp] = s1[rp] + d0[rp]
        for m in (0, 3, 1, 4):
            a_copy(half, rp, m).start()

    def finish_a():
        @pl.loop(0, 4)
        def _(p):
            for half in range(2):
                d_copy(p + 4 * half).wait_send()
                for m in range(6):
                    a_copy(half, p + 4 * half, m).wait_send()

    finish.append(finish_a)

    def combine_slice(half, rp):
        u = first[half]
        a_copy(half, rp, 0).wait_recv()
        cb[0, rp] = rb[0, rp] + s1[rp, :, mod(u + 1, 4), 0:8]
        a_copy(half, rp, 2).start()
        a_copy(half, rp, 3).wait_recv()
        cb[1, rp] = rb[3, rp] + s1[rp, :, mod(u + 3, 4), 8:16]
        a_copy(half, rp, 5).start()

    def second_slice(half, rp):
        u = first[half]
        for m in (1, 4, 2, 5):
            a_copy(half, rp, m).wait_recv()
        t1[rp, :, 0:8] = s1[rp, :, u, 0:8] + rb[4, rp] + rb[2, rp]
        t1[rp, :, 8:16] = s1[rp, :, u, 8:16] + rb[1, rp] + rb[5, rp]
        for m in range(3):
            b_copy(half, rp, m).start()

    def z_copy(rp):
        return remote(z1.at[rp], out.at[r], z_s.at[rp], z_r.at[r], at_z(rp))

    def last_slice(half, rp):
        for m in (1, 2, 0):
            b_copy(half, rp, m).wait_recv()
        total = t1[rp, second[half]] + rb2[1, rp] + rb2[2, rp] + rb2[0, rp]
        z1[rp] = total

        @pl.when(rp != r)
        def _():
            z_copy(rp).start()

    plan = (
        (make_slice, 0), (make_slice, 1), (send_slice, 0), (make_slice, 2), (send_slice, 1), (make_slice, 3),
        (send_slice, 2), (combine_slice, 0), (send_slice, 3), (combine_slice, 1), (combine_slice, 2),
        (second_slice, 0), (combine_slice, 3), (second_slice, 1), (second_slice, 2), (last_slice, 0),
        (second_slice, 3), (last_slice, 1), (last_slice, 2), (last_slice, 3),
    )
    for stage, p in plan:
        stage(0, p)
        stage(1, p + 4)

    out[r] = z1[r]

    @pl.loop(1, NZ)
    def _(k):
        source = mod(r + k, NZ)
        remote(z1.at[source], out.at[source], z_s.at[source], z_r.at[source], at_z(source)).wait_recv()

    for waits in finish:
        waits()

    @pl.loop(0, 4)
    def _(p):
        for half in range(2):
            for m in range(3):
                b_copy(half, p + 4 * half, m).wait_send()

    @pl.loop(1, NZ)
    def _(k):
        z_copy(mod(r + k, NZ)).wait_send()


def body(density, basis_values, grid_points, grid_weights, screened_blocks):
    vmem = pl.BlockSpec(memory_space=pltpu.VMEM)
    hbm = pl.BlockSpec(memory_space=pl.ANY)
    smem = pl.BlockSpec(memory_space=pltpu.SMEM)
    dma = pltpu.SemaphoreType.DMA
    rows = pl.pallas_call(
        kernel,
        out_shape=jax.ShapeDtypeStruct((8, 16, 512), F32),
        in_specs=[smem, hbm, hbm, vmem, vmem],
        out_specs=vmem,
        scratch_shapes=[
            pltpu.SMEM((2, 32), jnp.int32),
            pltpu.VMEM((4, 4, 2, 32, 16, 128), BF16),
            pltpu.VMEM((2, 17, 8, 16, 512), BF16),
            pltpu.VMEM((2, 16, 16, 2048), BF16),
            pltpu.VMEM((2, 4, 128, 128), F32),
            pltpu.VMEM((2, 64, 512), F32),
            pltpu.VMEM((2, 64, 128), F32),
            pltpu.VMEM((2, 8, 64, 256), BF16),
            pltpu.VMEM((2, 8, 64, 256), BF16),
            pltpu.VMEM((2, 8, 64, 256), BF16),
            pltpu.VMEM((2, 8, 64, 256), BF16),
            pltpu.VMEM((2, 256, 512), BF16),
            pltpu.VMEM((9, 32, 16, 512), BF16),
            pltpu.VMEM((8, 17, 16, 512), F32),
            pltpu.VMEM((2, 17, 16, 512), F32),
            pltpu.VMEM((8, 4, 4, 16, 512), F32),
            pltpu.VMEM((8, 4, 4, 16, 512), F32),
            pltpu.VMEM((8, 4, 4, 16, 512), F32),
            pltpu.VMEM((6, 8, 4, 8, 512), F32),
            pltpu.VMEM((2, 8, 4, 8, 512), F32),
            pltpu.VMEM((8, 4, 16, 512), F32),
            pltpu.VMEM((3, 8, 16, 512), F32),
            pltpu.VMEM((8, 16, 512), F32),
            dma((3,)),
            dma((2, 4, 2)), dma((2, 4, 2)),
            dma((2, 2, 2)), dma((2, 2, 2)),
            dma((4,)), dma((4,)),
            dma((2, 8)), dma((2, 8)),
            dma((2, 8)), dma((2, 8)),
            dma((8,)), dma((8,)),
            dma((6, 8)), dma((6, 8)),
            dma((3, 8)), dma((3, 8)),
            dma((8,)), dma((8,)),
        ],
        compiler_params=pltpu.CompilerParams(
            collective_id=0, has_side_effects=True, vmem_limit_bytes=60 * 1024 * 1024
        ),
        cost_estimate=pl.CostEstimate(flops=4_000_000_000, bytes_accessed=2_000_000, transcendentals=100_000),
        name="exchange",
    )(screened_blocks, density, basis_values, jnp.transpose(grid_points, (1, 0, 2)), grid_weights)
    return rows.reshape(128, 512).T.reshape(32, 16, 128)


def solution(mesh):
    placed = (
        P(None, "rows", "grid"),
        P("grid", None, "rows", None),
        P("grid", None, None),
        P("grid", None),
        P("grid", None),
    )
    return jax.shard_map(
        body, mesh=mesh, in_specs=placed, out_specs=P(None, "rows", "grid"), check_vma=False
    )
```

```python
import jax
import jax.numpy as jnp
from jax import lax
from jax.experimental import pallas as pl
from jax.experimental.pallas import tpu as pltpu
from jax.sharding import PartitionSpec as P

MESH = pl.DeviceIdType.MESH
NX = 4
NY = 4
NZ = 8
BF16 = jnp.bfloat16
F32 = jnp.float32
NT = (((1,), (1,)), ((), ()))
FAR_FIRST = (4, 3, 5, 2, 6, 1, 7)
LIMIT = 32767.0
TINY = 1e-33


def mod(a, n):
    return lax.rem(a, n)


def encode(values, codes, scales):
    largest = jnp.max(jnp.abs(values), axis=0, keepdims=True)
    codes[...] = jnp.round(values * (LIMIT / jnp.maximum(largest, TINY))).astype(jnp.int32).astype(jnp.int16)
    scales[...] = largest * (1.0 / LIMIT)


def decode(codes, scales):
    return codes[...].astype(jnp.int32).astype(F32) * scales[...]


def kernel(
    sel, dens, xin, pts, wts, out,
    inv, pg, xg, psel, tcol, scale, wcol, fs, fr, ps, pr, pot, xd, k0, k1, kp, kq, ks, s1, aq, az, t1, bq, bz, z1,
    o_s, x_s, x_r, p_s, p_r, q_s, q_r, f_s, f_r, m_s, m_r, d_s, d_r, a_s, a_r, b_s, b_r, z_s, z_r,
):
    g = lax.axis_index("grid")
    r = lax.axis_index("rows")
    core = mod(g, 2)
    chip = lax.div(g, 2)
    x = mod(chip, NX)
    y = lax.div(chip, NX)
    finish = []

    def at_plane(xx, yy):
        return (2 * (NX * yy + xx) + core, r)

    def at_z(rr):
        return (g, rr)

    partner = (2 * chip + 1 - core, r)
    up, down = at_z(mod(r + 1, NZ)), at_z(mod(r + NZ - 1, NZ))
    east, west = at_plane(mod(x + 1, NX), y), at_plane(mod(x + NX - 1, NX), y)
    north, south = at_plane(x, mod(y + 1, NY)), at_plane(x, mod(y + NY - 1, NY))

    def remote(src, dst, send, recv, device):
        return pltpu.make_async_remote_copy(
            src_ref=src, dst_ref=dst, send_sem=send, recv_sem=recv, device_id=device, device_id_type=MESH
        )

    own = [pltpu.make_async_copy(xin.at[b], xg.at[b, pl.ds(0, 16), r], o_s.at[b]) for b in range(2)]
    own.append(pltpu.make_async_copy(dens, pg.at[y, x, core], o_s.at[2]))
    for copy in own:
        copy.start()
    bar = pltpu.get_barrier_semaphore()
    for device in (up, down, east, west, north, south, partner):
        pl.semaphore_signal(bar, inc=1, device_id=device, device_id_type=MESH)
    pl.semaphore_wait(bar, 7)
    own[0].wait()

    def x_copy(d, t, b):
        shard = mod(r + (NZ - t if d == 0 else t), NZ)
        part = pl.ds(0, 16) if t < 3 else pl.ds(8 * d, 8)
        dst = xg.at[b, part, shard]
        return remote(dst, dst, x_s.at[d, t, b], x_r.at[d, t, b], up if d == 0 else down)

    def x_send(t, b):
        for d in range(2):
            if t > 0:
                x_copy(d, t - 1, b).wait_recv()
            x_copy(d, t, b).start()

    def px_copy(d, t):
        if t == 0:
            ref = pg.at[y, x, core]
        else:
            ref = pg.at[y, mod(x + (3 if d == 0 else 1), NX), core, pl.ds(16 * d, 16)]
        return remote(ref, ref, p_s.at[0, d, t], p_r.at[0, d, t], east if d == 0 else west)

    def py_copy(d, t):
        if t == 0:
            ref = pg.at[y, :, core]
        else:
            ref = pg.at[mod(y + (3 if d == 0 else 1), NY), :, core, pl.ds(16 * d, 16)]
        return remote(ref, ref, p_s.at[1, d, t], p_r.at[1, d, t], north if d == 0 else south)

    def pq_copy(k):
        ref = pg.at[mod(y + k, NY), :, core]
        return remote(ref, ref, q_s.at[k], q_r.at[k], partner)

    x_send(0, 0)
    own[2].wait()
    px_copy(0, 0).start()
    px_copy(1, 0).start()
    own[1].wait()
    x_send(0, 1)

    for rp in range(8):
        k0[rp, 16] = jnp.zeros(k0.shape[2:], F32)
    for half in range(2):
        k1[half, 16] = jnp.zeros(k1.shape[2:], F32)
    for b in range(2):
        xg[b, 16] = jnp.zeros(xg.shape[2:], BF16)

    px_copy(0, 0).wait_recv()
    px_copy(0, 1).start()
    px_copy(1, 0).wait_recv()
    px_copy(1, 1).start()

    @pl.loop(0, 32)
    def _(nb):
        for b in range(2):
            at = jnp.int32(16)
            for s in range(16):
                at = jnp.where(sel[b, s] == nb, s, at)
            inv[b, nb] = at

    x_send(1, 0)

    px_copy(0, 1).wait_recv()
    px_copy(1, 1).wait_recv()
    py_copy(0, 0).start()
    py_copy(1, 0).start()
    pq_copy(0).start()

    lanes = pl.ds(pl.multiple_of(128 * lax.div(r, 2), 128), 128)
    mine = pl.ds(pl.multiple_of(64 * mod(r, 2), 64), 64)
    for b in range(2):
        for c in range(4):
            row = pts[c, b : b + 1, lanes] if c < 3 else wts[b : b + 1, lanes]
            tcol[b, c] = jnp.broadcast_to(row, (128, 128)).T
        dist = jnp.zeros((64, 512), F32)
        for c in range(3):
            diff = pts[c, b : b + 1, :] - jnp.concatenate([tcol[b, c, mine]] * 4, axis=1)
            dist = dist + diff * diff
        scale[b] = wts[b : b + 1, :] * (1.0 / jnp.sqrt(dist + 0.5))
        wcol[b] = tcol[b, 3, mine]

    x_send(1, 1)
    x_send(2, 0)

    for d in range(2):
        py_copy(d, 0).wait_recv()
        py_copy(d, 1).start()
    pq_copy(1).start()
    pq_copy(3).start()

    x_send(2, 1)
    x_send(3, 0)

    py_copy(0, 1).wait_recv()
    py_copy(1, 1).wait_recv()
    pq_copy(2).start()

    x_send(3, 1)

    for k in range(4):
        pq_copy(k).wait_recv()

    def finish_gathers():
        for d in range(2):
            for t in range(4):
                for b in range(2):
                    x_copy(d, t, b).wait_send()
            for t in range(2):
                px_copy(d, t).wait_send()
                py_copy(d, t).wait_send()
        for k in range(4):
            pq_copy(k).wait_send()

    finish.append(finish_gathers)

    @pl.loop(0, 16)
    def _(s):
        for b in range(2):
            row = sel[b, s]
            for c in range(16):
                col = sel[b, c]
                psel[b, s, :, 128 * c : 128 * (c + 1)] = pg[
                    lax.div(col, 8), mod(lax.div(col, 2), 4), mod(col, 2), row
                ]

    def f_copy(b, k):
        to = mod(r + k, NZ)
        return remote(fs.at[b, to], fr.at[b, r], f_s.at[b, k], f_r.at[b, k], at_z(to))

    for b in range(2):
        for d in range(2):
            x_copy(d, 3, b).wait_recv()
        f = jnp.dot(
            psel[b].reshape(256, 2048), xg[b, 0:16].reshape(2048, 512), preferred_element_type=F32
        ).astype(BF16)
        fs[b] = f.T.reshape(8, 64, 256)
        for k in FAR_FIRST:
            f_copy(b, k).start()
        fr[b, r] = fs[b, r]

    def finish_f():
        for b in range(2):
            for k in FAR_FIRST:
                f_copy(b, k).wait_send()

    finish.append(finish_f)

    def m_copy(b, k):
        to = mod(r + k, NZ)
        return remote(ps.at[b, to], pr.at[b, r], m_s.at[b, k], m_r.at[b, k], at_z(to))

    for b in range(2):
        for k in FAR_FIRST:
            f_copy(b, k).wait_recv()
        inter = jnp.zeros((64, 512), F32)
        for s in range(8):
            inter = inter + jnp.dot(fr[b, s], xg[b, 0:16, s].reshape(256, 512), preferred_element_type=F32)
        mixed = (scale[b] * inter).astype(BF16)
        factor = jnp.concatenate([wcol[b]] * 2, axis=1)
        for s in range(8):
            p = lax.dot_general(mixed, xg[b, 0:16, s].reshape(256, 512), NT, preferred_element_type=F32)
            ps[b, s] = (p * factor).astype(BF16)
        for k in FAR_FIRST:
            m_copy(b, k).start()
        pr[b, r] = ps[b, r]

    def finish_m():
        for b in range(2):
            for k in FAR_FIRST:
                m_copy(b, k).wait_send()

    finish.append(finish_m)

    def potential(b):
        for k in FAR_FIRST:
            m_copy(b, k).wait_recv()
        pot[b] = pr[b].reshape(512, 256).T

    potential(0)

    @pl.loop(0, 8)
    def _(rp):
        for a in range(32):
            xd[8, a] = xg[0, inv[0, a], rp]
        k0[rp, 0:16] = lax.dot_general(
            pot[0], xd[8].reshape(512, 512), NT, preferred_element_type=F32
        ).reshape(16, 16, 512)
        for a in range(32):
            xd[rp, a] = xg[1, inv[1, a], rp]

    potential(1)

    first = (x, y)
    second = (y, x)

    def pair(codes, scales, code_sems, scale_sems, device):
        return (remote(*codes, *code_sems, device), remote(*scales, *scale_sems, device))

    def d_copy(rp):
        return pair(
            (kq.at[0, rp], kq.at[1, rp]), (ks.at[0, rp], ks.at[1, rp]),
            (d_s.at[0, rp], d_r.at[0, rp]), (d_s.at[1, rp], d_r.at[1, rp]), partner,
        )

    def start(copies):
        for copy in copies:
            copy.start()

    def wait_recv(copies):
        for copy in copies:
            copy.wait_recv()

    def wait_send(copies):
        for copy in copies:
            copy.wait_send()

    def along(half, stage, shift):
        if half == stage:
            return at_plane(mod(x + shift, NX), y)
        return at_plane(x, mod(y + shift, NY))

    def a_copy(half, rp, m):
        return pair(
            (aq.at[0, m, rp], aq.at[1, m, rp]), (az.at[0, m, rp], az.at[1, m, rp]),
            (a_s.at[0, m, rp], a_r.at[0, m, rp]), (a_s.at[1, m, rp], a_r.at[1, m, rp]),
            along(half, 0, 1 if m < 3 else 3),
        )

    def a_send(half, rp, m, values):
        encode(values.reshape(32, 512), aq.at[0, m, rp], az.at[0, m, rp])
        start(a_copy(half, rp, m))

    def a_value(rp, m):
        return decode(aq.at[1, m, rp], az.at[1, m, rp]).reshape(4, 8, 512)

    def b_copy(half, rp, m):
        return pair(
            (bq.at[0, m, rp], bq.at[1, m, rp]), (bz.at[0, m, rp], bz.at[1, m, rp]),
            (b_s.at[0, m, rp], b_r.at[0, m, rp]), (b_s.at[1, m, rp], b_r.at[1, m, rp]),
            along(half, 1, (2, 1, 3)[m]),
        )

    def make_slice(half, rp):
        k1[half, 0:16] = lax.dot_general(
            pot[1], xd[rp].reshape(512, 512), NT, preferred_element_type=F32
        ).reshape(16, 16, 512)
        for ref, c in ((kp, 1 - core), (s1, core)):
            for v in range(4):
                for u in range(4):
                    nb = 2 * (NX * v + u if half == 0 else NX * u + v) + c
                    ref[rp, v, u] = k0[rp, inv[0, nb]] + k1[half, inv[1, nb]]
            if ref is kp:
                for part in range(8):
                    encode(
                        kp[rp, part // 2, 2 * (part % 2) : 2 * (part % 2) + 2].reshape(32, 512),
                        kq.at[0, rp, pl.ds(32 * part, 32)], ks.at[0, rp, part],
                    )
                start(d_copy(rp))

    def send_slice(half, rp):
        wait_recv(d_copy(rp))
        for part in range(8):
            s1[rp, part // 2, 2 * (part % 2) : 2 * (part % 2) + 2] += decode(
                kq.at[1, rp, pl.ds(32 * part, 32)], ks.at[1, rp, part]
            ).reshape(2, 16, 512)
        u = first[half]
        a_send(half, rp, 0, s1[rp, :, mod(u + 2, 4), 0:8])
        a_send(half, rp, 3, s1[rp, :, mod(u + 2, 4), 8:16])
        a_send(half, rp, 1, s1[rp, :, mod(u + 1, 4), 8:16])
        a_send(half, rp, 4, s1[rp, :, mod(u + 3, 4), 0:8])

    def finish_a():
        @pl.loop(0, 4)
        def _(p):
            for half in range(2):
                wait_send(d_copy(p + 4 * half))
                for m in range(6):
                    wait_send(a_copy(half, p + 4 * half, m))

    finish.append(finish_a)

    def combine_slice(half, rp):
        u = first[half]
        wait_recv(a_copy(half, rp, 0))
        a_send(half, rp, 2, a_value(rp, 0) + s1[rp, :, mod(u + 1, 4), 0:8])
        wait_recv(a_copy(half, rp, 3))
        a_send(half, rp, 5, a_value(rp, 3) + s1[rp, :, mod(u + 3, 4), 8:16])

    def second_slice(half, rp):
        u = first[half]
        for m in (1, 4, 2, 5):
            wait_recv(a_copy(half, rp, m))
        t1[rp, :, 0:8] = s1[rp, :, u, 0:8] + a_value(rp, 4) + a_value(rp, 2)
        t1[rp, :, 8:16] = s1[rp, :, u, 8:16] + a_value(rp, 1) + a_value(rp, 5)
        for m in range(3):
            encode(t1[rp, mod(second[half] + (2, 1, 3)[m], 4)], bq.at[0, m, rp], bz.at[0, m, rp])
            start(b_copy(half, rp, m))

    def z_copy(rp):
        return remote(z1.at[rp], out.at[r], z_s.at[rp], z_r.at[r], at_z(rp))

    def last_slice(half, rp):
        total = t1[rp, second[half]]
        for m in (1, 2, 0):
            wait_recv(b_copy(half, rp, m))
            total = total + decode(bq.at[1, m, rp], bz.at[1, m, rp])
        z1[rp] = total

        @pl.when(rp != r)
        def _():
            z_copy(rp).start()

    plan = (
        (make_slice, 0), (make_slice, 1), (send_slice, 0), (make_slice, 2), (send_slice, 1), (make_slice, 3),
        (send_slice, 2), (combine_slice, 0), (send_slice, 3), (combine_slice, 1), (combine_slice, 2),
        (second_slice, 0), (combine_slice, 3), (second_slice, 1), (second_slice, 2), (last_slice, 0),
        (second_slice, 3), (last_slice, 1), (last_slice, 2), (last_slice, 3),
    )
    for stage, p in plan:
        stage(0, p)
        stage(1, p + 4)

    out[r] = z1[r]

    @pl.loop(1, NZ)
    def _(k):
        source = mod(r + k, NZ)
        remote(z1.at[source], out.at[source], z_s.at[source], z_r.at[source], at_z(source)).wait_recv()

    for waits in finish:
        waits()

    @pl.loop(0, 4)
    def _(p):
        for half in range(2):
            for m in range(3):
                wait_send(b_copy(half, p + 4 * half, m))

    @pl.loop(1, NZ)
    def _(k):
        z_copy(mod(r + k, NZ)).wait_send()


def body(density, basis_values, grid_points, grid_weights, screened_blocks):
    vmem = pl.BlockSpec(memory_space=pltpu.VMEM)
    hbm = pl.BlockSpec(memory_space=pl.ANY)
    smem = pl.BlockSpec(memory_space=pltpu.SMEM)
    dma = pltpu.SemaphoreType.DMA
    rows = pl.pallas_call(
        kernel,
        out_shape=jax.ShapeDtypeStruct((8, 16, 512), F32),
        in_specs=[smem, hbm, hbm, vmem, vmem],
        out_specs=vmem,
        scratch_shapes=[
            pltpu.SMEM((2, 32), jnp.int32),
            pltpu.VMEM((4, 4, 2, 32, 16, 128), BF16),
            pltpu.VMEM((2, 17, 8, 16, 512), BF16),
            pltpu.VMEM((2, 16, 16, 2048), BF16),
            pltpu.VMEM((2, 4, 128, 128), F32),
            pltpu.VMEM((2, 64, 512), F32),
            pltpu.VMEM((2, 64, 128), F32),
            pltpu.VMEM((2, 8, 64, 256), BF16),
            pltpu.VMEM((2, 8, 64, 256), BF16),
            pltpu.VMEM((2, 8, 64, 256), BF16),
            pltpu.VMEM((2, 8, 64, 256), BF16),
            pltpu.VMEM((2, 256, 512), BF16),
            pltpu.VMEM((9, 32, 16, 512), BF16),
            pltpu.VMEM((8, 17, 16, 512), F32),
            pltpu.VMEM((2, 17, 16, 512), F32),
            pltpu.VMEM((8, 4, 4, 16, 512), F32),
            pltpu.VMEM((2, 8, 256, 512), jnp.int16),
            pltpu.VMEM((2, 8, 8, 1, 512), F32),
            pltpu.VMEM((8, 4, 4, 16, 512), F32),
            pltpu.VMEM((2, 6, 8, 32, 512), jnp.int16),
            pltpu.VMEM((2, 6, 8, 1, 512), F32),
            pltpu.VMEM((8, 4, 16, 512), F32),
            pltpu.VMEM((2, 3, 8, 16, 512), jnp.int16),
            pltpu.VMEM((2, 3, 8, 1, 512), F32),
            pltpu.VMEM((8, 16, 512), F32),
            dma((3,)),
            dma((2, 4, 2)), dma((2, 4, 2)),
            dma((2, 2, 2)), dma((2, 2, 2)),
            dma((4,)), dma((4,)),
            dma((2, 8)), dma((2, 8)),
            dma((2, 8)), dma((2, 8)),
            dma((2, 8)), dma((2, 8)),
            dma((2, 6, 8)), dma((2, 6, 8)),
            dma((2, 3, 8)), dma((2, 3, 8)),
            dma((8,)), dma((8,)),
        ],
        compiler_params=pltpu.CompilerParams(
            collective_id=0, has_side_effects=True, vmem_limit_bytes=60 * 1024 * 1024
        ),
        cost_estimate=pl.CostEstimate(flops=4_000_000_000, bytes_accessed=2_000_000, transcendentals=100_000),
        name="exchange",
    )(screened_blocks, density, basis_values, jnp.transpose(grid_points, (1, 0, 2)), grid_weights)
    return rows.reshape(128, 512).T.reshape(32, 16, 128)


def solution(mesh):
    placed = (
        P(None, "rows", "grid"),
        P("grid", None, "rows", None),
        P("grid", None, None),
        P("grid", None),
        P("grid", None),
    )
    return jax.shard_map(
        body, mesh=mesh, in_specs=placed, out_specs=P(None, "rows", "grid"), check_vma=False
    )
```

```python
import jax
import jax.numpy as jnp
from jax import lax
from jax.experimental import pallas as pl
from jax.experimental.pallas import tpu as pltpu
from jax.sharding import PartitionSpec as P

MESH = pl.DeviceIdType.MESH
NX = 4
NY = 4
NZ = 8
BF16 = jnp.bfloat16
F32 = jnp.float32
NT = (((1,), (1,)), ((), ()))
FAR_FIRST = (4, 3, 5, 2, 6, 1, 7)
LIMIT = 32767.0
TINY = 1.2e-38


def mod(a, n):
    return lax.rem(a, n)


def encode(values, codes, scales):
    largest = jnp.max(jnp.abs(values), axis=0, keepdims=True)
    parts = values * (1.0 / jnp.maximum(largest, TINY))
    codes[...] = jnp.round(parts * LIMIT).astype(jnp.int32).astype(jnp.int16)
    scales[...] = largest


def decode(codes, scales):
    return (codes[...].astype(jnp.int32).astype(F32) * (1.0 / LIMIT)) * scales[...]


def kernel(
    sel, dens, xin, pts, wts, out,
    inv, pg, xg, psel, tcol, scale, wcol, fs, fr, ps, pr, pot, xd, k0, k1, kp, kq, ks, s1, aq, az, t1, bq, bz, z1,
    o_s, x_s, x_r, p_s, p_r, q_s, q_r, f_s, f_r, m_s, m_r, d_s, d_r, a_s, a_r, b_s, b_r, z_s, z_r,
):
    g = lax.axis_index("grid")
    r = lax.axis_index("rows")
    core = mod(g, 2)
    chip = lax.div(g, 2)
    x = mod(chip, NX)
    y = lax.div(chip, NX)
    finish = []

    def at_plane(xx, yy):
        return (2 * (NX * yy + xx) + core, r)

    def at_z(rr):
        return (g, rr)

    partner = (2 * chip + 1 - core, r)
    up, down = at_z(mod(r + 1, NZ)), at_z(mod(r + NZ - 1, NZ))
    east, west = at_plane(mod(x + 1, NX), y), at_plane(mod(x + NX - 1, NX), y)
    north, south = at_plane(x, mod(y + 1, NY)), at_plane(x, mod(y + NY - 1, NY))

    def remote(src, dst, send, recv, device):
        return pltpu.make_async_remote_copy(
            src_ref=src, dst_ref=dst, send_sem=send, recv_sem=recv, device_id=device, device_id_type=MESH
        )

    own = [pltpu.make_async_copy(xin.at[b], xg.at[b, pl.ds(0, 16), r], o_s.at[b]) for b in range(2)]
    own.append(pltpu.make_async_copy(dens, pg.at[y, x, core], o_s.at[2]))
    for copy in own:
        copy.start()
    bar = pltpu.get_barrier_semaphore()
    for device in (up, down, east, west, north, south, partner):
        pl.semaphore_signal(bar, inc=1, device_id=device, device_id_type=MESH)
    pl.semaphore_wait(bar, 7)
    own[0].wait()

    def x_copy(d, t, b):
        shard = mod(r + (NZ - t if d == 0 else t), NZ)
        part = pl.ds(0, 16) if t < 3 else pl.ds(8 * d, 8)
        dst = xg.at[b, part, shard]
        return remote(dst, dst, x_s.at[0], x_r.at[d, t, b], up if d == 0 else down)

    def x_send(t, b):
        for d in range(2):
            if t > 0:
                x_copy(d, t - 1, b).wait_recv()
            x_copy(d, t, b).start()

    def px_copy(d, t):
        if t == 0:
            ref = pg.at[y, x, core]
        else:
            ref = pg.at[y, mod(x + (3 if d == 0 else 1), NX), core, pl.ds(16 * d, 16)]
        return remote(ref, ref, p_s.at[0, d, t], p_r.at[0, d, t], east if d == 0 else west)

    def py_copy(d, t):
        if t == 0:
            ref = pg.at[y, :, core]
        else:
            ref = pg.at[mod(y + (3 if d == 0 else 1), NY), :, core, pl.ds(16 * d, 16)]
        return remote(ref, ref, p_s.at[1, d, t], p_r.at[1, d, t], north if d == 0 else south)

    def pq_copy(k):
        ref = pg.at[mod(y + k, NY), :, core]
        return remote(ref, ref, q_s.at[k], q_r.at[k], partner)

    x_send(0, 0)
    own[2].wait()
    px_copy(0, 0).start()
    px_copy(1, 0).start()
    own[1].wait()
    x_send(0, 1)

    for rp in range(8):
        k0[rp, 16] = jnp.zeros(k0.shape[2:], F32)
    for half in range(2):
        k1[half, 16] = jnp.zeros(k1.shape[2:], F32)
    for b in range(2):
        xg[b, 16] = jnp.zeros(xg.shape[2:], BF16)

    px_copy(0, 0).wait_recv()
    px_copy(0, 1).start()
    px_copy(1, 0).wait_recv()
    px_copy(1, 1).start()

    @pl.loop(0, 32)
    def _(nb):
        for b in range(2):
            at = jnp.int32(16)
            for s in range(16):
                at = jnp.where(sel[b, s] == nb, s, at)
            inv[b, nb] = at

    x_send(1, 0)

    px_copy(0, 1).wait_recv()
    px_copy(1, 1).wait_recv()
    py_copy(0, 0).start()
    py_copy(1, 0).start()
    pq_copy(0).start()

    lanes = pl.ds(pl.multiple_of(128 * lax.div(r, 2), 128), 128)
    mine = pl.ds(pl.multiple_of(64 * mod(r, 2), 64), 64)
    for b in range(2):
        for c in range(4):
            row = pts[c, b : b + 1, lanes] if c < 3 else wts[b : b + 1, lanes]
            tcol[b, c] = jnp.broadcast_to(row, (128, 128)).T
        dist = jnp.zeros((64, 512), F32)
        for c in range(3):
            diff = pts[c, b : b + 1, :] - jnp.concatenate([tcol[b, c, mine]] * 4, axis=1)
            dist = dist + diff * diff
        scale[b] = wts[b : b + 1, :] * (1.0 / jnp.sqrt(dist + 0.5))
        wcol[b] = tcol[b, 3, mine]

    x_send(1, 1)
    x_send(2, 0)

    for d in range(2):
        py_copy(d, 0).wait_recv()
        py_copy(d, 1).start()
    pq_copy(1).start()
    pq_copy(3).start()

    x_send(2, 1)
    x_send(3, 0)

    py_copy(0, 1).wait_recv()
    py_copy(1, 1).wait_recv()
    pq_copy(2).start()

    x_send(3, 1)

    for k in range(4):
        pq_copy(k).wait_recv()

    def finish_gathers():
        sent = xg.at[:, pl.ds(0, 16), pl.ds(0, 7)]
        remote(sent, sent, x_s.at[0], x_r.at[0, 0, 0], up).wait_send()
        for d in range(2):
            for t in range(2):
                px_copy(d, t).wait_send()
                py_copy(d, t).wait_send()
        for k in range(4):
            pq_copy(k).wait_send()

    finish.append(finish_gathers)

    @pl.loop(0, 16)
    def _(s):
        for b in range(2):
            row = sel[b, s]
            for c in range(16):
                col = sel[b, c]
                psel[b, s, :, 128 * c : 128 * (c + 1)] = pg[
                    lax.div(col, 8), mod(lax.div(col, 2), 4), mod(col, 2), row
                ]

    def f_copy(b, k):
        to = mod(r + k, NZ)
        return remote(fs.at[b, to], fr.at[b, r], f_s.at[0], f_r.at[b], at_z(to))

    for b in range(2):
        for d in range(2):
            x_copy(d, 3, b).wait_recv()
        f = jnp.dot(
            psel[b].reshape(256, 2048), xg[b, 0:16].reshape(2048, 512), preferred_element_type=F32
        ).astype(BF16)
        fs[b] = f.T.reshape(8, 64, 256)
        for k in FAR_FIRST:
            f_copy(b, k).start()
        fr[b, r] = fs[b, r]

    def finish_f():
        some = pl.ds(0, 7)
        remote(fs.at[:, some], fr.at[:, some], f_s.at[0], f_r.at[0], up).wait_send()

    finish.append(finish_f)

    def m_copy(b, k):
        to = mod(r + k, NZ)
        return remote(ps.at[b, to], pr.at[b, r], m_s.at[0], m_r.at[b], at_z(to))

    for b in range(2):
        remote(fs.at[b, pl.ds(0, 7)], fr.at[b, pl.ds(0, 7)], f_s.at[0], f_r.at[b], up).wait_recv()
        inter = jnp.zeros((64, 512), F32)
        for s in range(8):
            inter = inter + jnp.dot(fr[b, s], xg[b, 0:16, s].reshape(256, 512), preferred_element_type=F32)
        mixed = (scale[b] * inter).astype(BF16)
        factor = jnp.concatenate([wcol[b]] * 2, axis=1)
        for s in range(8):
            p = lax.dot_general(mixed, xg[b, 0:16, s].reshape(256, 512), NT, preferred_element_type=F32)
            ps[b, s] = (p * factor).astype(BF16)
        for k in FAR_FIRST:
            m_copy(b, k).start()
        pr[b, r] = ps[b, r]

    def finish_m():
        some = pl.ds(0, 7)
        remote(ps.at[:, some], pr.at[:, some], m_s.at[0], m_r.at[0], up).wait_send()

    finish.append(finish_m)

    def potential(b):
        remote(ps.at[b, pl.ds(0, 7)], pr.at[b, pl.ds(0, 7)], m_s.at[0], m_r.at[b], up).wait_recv()
        pot[b] = pr[b].reshape(512, 256).T

    potential(0)

    @pl.loop(0, 8)
    def _(rp):
        for a in range(32):
            xd[8, a] = xg[0, inv[0, a], rp]
        k0[rp, 0:16] = lax.dot_general(
            pot[0], xd[8].reshape(512, 512), NT, preferred_element_type=F32
        ).reshape(16, 16, 512)
        for a in range(32):
            xd[rp, a] = xg[1, inv[1, a], rp]

    potential(1)

    first = (x, y)
    second = (y, x)

    def pair(codes, scales, code_sems, scale_sems, device):
        return (remote(*codes, *code_sems, device), remote(*scales, *scale_sems, device))

    def d_copy(rp):
        return pair(
            (kq.at[0, rp], kq.at[1, rp]), (ks.at[0, rp], ks.at[1, rp]),
            (d_s.at[0], d_r.at[0, rp]), (d_s.at[1], d_r.at[1, rp]), partner,
        )

    def start(copies):
        for copy in copies:
            copy.start()

    def wait_recv(copies):
        for copy in copies:
            copy.wait_recv()

    def wait_send(copies):
        for copy in copies:
            copy.wait_send()

    def along(half, stage, shift):
        if half == stage:
            return at_plane(mod(x + shift, NX), y)
        return at_plane(x, mod(y + shift, NY))

    def a_pair(rp, which, group, device):
        return pair(
            (aq.at[0, which, rp], aq.at[1, which, rp]), (az.at[0, which, rp], az.at[1, which, rp]),
            (a_s.at[0], a_r.at[0, group, rp]), (a_s.at[1], a_r.at[1, group, rp]), device,
        )

    def a_send(half, rp, m, values):
        encode(values.reshape(32, 512), aq.at[0, m, rp], az.at[0, m, rp])
        start(a_pair(rp, m, min(m, 2), along(half, 0, 1 if m % 2 == 0 else 3)))

    def a_value(rp, m):
        return decode(aq.at[1, m, rp], az.at[1, m, rp]).reshape(4, 8, 512)

    def b_pair(rp, which, device):
        return pair(
            (bq.at[0, which, rp], bq.at[1, which, rp]), (bz.at[0, which, rp], bz.at[1, which, rp]),
            (b_s.at[0], b_r.at[0, rp]), (b_s.at[1], b_r.at[1, rp]), device,
        )

    def make_slice(half, rp):
        k1[half, 0:16] = lax.dot_general(
            pot[1], xd[rp].reshape(512, 512), NT, preferred_element_type=F32
        ).reshape(16, 16, 512)
        for ref, c in ((kp, 1 - core), (s1, core)):
            for v in range(4):
                for u in range(4):
                    nb = 2 * (NX * v + u if half == 0 else NX * u + v) + c
                    ref[rp, v, u] = k0[rp, inv[0, nb]] + k1[half, inv[1, nb]]
            if ref is kp:
                for part in range(8):
                    encode(
                        kp[rp, part // 2, 2 * (part % 2) : 2 * (part % 2) + 2].reshape(32, 512),
                        kq.at[0, rp, pl.ds(32 * part, 32)], ks.at[0, rp, part],
                    )
                start(d_copy(rp))

    def send_slice(half, rp):
        wait_recv(d_copy(rp))
        for part in range(8):
            s1[rp, part // 2, 2 * (part % 2) : 2 * (part % 2) + 2] += decode(
                kq.at[1, rp, pl.ds(32 * part, 32)], ks.at[1, rp, part]
            ).reshape(2, 16, 512)
        u = first[half]
        a_send(half, rp, 0, s1[rp, :, mod(u + 2, 4), 0:8])
        a_send(half, rp, 1, s1[rp, :, mod(u + 2, 4), 8:16])
        a_send(half, rp, 2, s1[rp, :, mod(u + 1, 4), 8:16])
        a_send(half, rp, 3, s1[rp, :, mod(u + 3, 4), 0:8])

    def finish_a():
        def whole(codes, scales, send, recv):
            first_of = (0,) * (len(recv.shape) - 1)
            wait_send(
                pair(
                    (codes.at[0], codes.at[1]), (scales.at[0], scales.at[1]),
                    (send.at[0], recv.at[(0, *first_of)]), (send.at[1], recv.at[(1, *first_of)]), partner,
                )
            )

        whole(kq, ks, d_s, d_r)
        whole(aq, az, a_s, a_r)
        whole(bq, bz, b_s, b_r)

    finish.append(finish_a)

    def combine_slice(half, rp):
        u = first[half]
        wait_recv(a_pair(rp, 0, 0, partner))
        a_send(half, rp, 4, a_value(rp, 0) + s1[rp, :, mod(u + 1, 4), 0:8])
        wait_recv(a_pair(rp, 1, 1, partner))
        a_send(half, rp, 5, a_value(rp, 1) + s1[rp, :, mod(u + 3, 4), 8:16])

    def second_slice(half, rp):
        u = first[half]
        wait_recv(a_pair(rp, pl.ds(2, 4), 2, partner))
        t1[rp, :, 0:8] = s1[rp, :, u, 0:8] + a_value(rp, 3) + a_value(rp, 4)
        t1[rp, :, 8:16] = s1[rp, :, u, 8:16] + a_value(rp, 2) + a_value(rp, 5)
        for m in range(3):
            encode(t1[rp, mod(second[half] + (2, 1, 3)[m], 4)], bq.at[0, m, rp], bz.at[0, m, rp])
            start(b_pair(rp, m, along(half, 1, (2, 1, 3)[m])))

    def z_copy(rp):
        return remote(z1.at[rp], out.at[r], z_s.at[0], z_r.at[0], at_z(rp))

    def last_slice(half, rp):
        total = t1[rp, second[half]]
        wait_recv(b_pair(rp, pl.ds(0, 3), partner))
        for m in range(3):
            total = total + decode(bq.at[1, m, rp], bz.at[1, m, rp])
        z1[rp] = total

        @pl.when(rp != r)
        def _():
            z_copy(rp).start()

    plan = (
        (make_slice, 0), (make_slice, 1), (send_slice, 0), (make_slice, 2), (send_slice, 1), (make_slice, 3),
        (send_slice, 2), (combine_slice, 0), (send_slice, 3), (combine_slice, 1), (combine_slice, 2),
        (second_slice, 0), (combine_slice, 3), (second_slice, 1), (second_slice, 2), (last_slice, 0),
        (second_slice, 3), (last_slice, 1), (last_slice, 2), (last_slice, 3),
    )
    for stage, p in plan:
        stage(0, p)
        stage(1, p + 4)

    out[r] = z1[r]

    others = remote(z1.at[pl.ds(0, 7)], out.at[pl.ds(0, 7)], z_s.at[0], z_r.at[0], up)
    others.wait_recv()

    for waits in finish:
        waits()

    others.wait_send()


def body(density, basis_values, grid_points, grid_weights, screened_blocks):
    vmem = pl.BlockSpec(memory_space=pltpu.VMEM)
    hbm = pl.BlockSpec(memory_space=pl.ANY)
    smem = pl.BlockSpec(memory_space=pltpu.SMEM)
    dma = pltpu.SemaphoreType.DMA
    rows = pl.pallas_call(
        kernel,
        out_shape=jax.ShapeDtypeStruct((8, 16, 512), F32),
        in_specs=[smem, hbm, hbm, vmem, vmem],
        out_specs=vmem,
        scratch_shapes=[
            pltpu.SMEM((2, 32), jnp.int32),
            pltpu.VMEM((4, 4, 2, 32, 16, 128), BF16),
            pltpu.VMEM((2, 17, 8, 16, 512), BF16),
            pltpu.VMEM((2, 16, 16, 2048), BF16),
            pltpu.VMEM((2, 4, 128, 128), F32),
            pltpu.VMEM((2, 64, 512), F32),
            pltpu.VMEM((2, 64, 128), F32),
            pltpu.VMEM((2, 8, 64, 256), BF16),
            pltpu.VMEM((2, 8, 64, 256), BF16),
            pltpu.VMEM((2, 8, 64, 256), BF16),
            pltpu.VMEM((2, 8, 64, 256), BF16),
            pltpu.VMEM((2, 256, 512), BF16),
            pltpu.VMEM((9, 32, 16, 512), BF16),
            pltpu.VMEM((8, 17, 16, 512), F32),
            pltpu.VMEM((2, 17, 16, 512), F32),
            pltpu.VMEM((8, 4, 4, 16, 512), F32),
            pltpu.VMEM((2, 8, 256, 512), jnp.int16),
            pltpu.VMEM((2, 8, 8, 1, 512), F32),
            pltpu.VMEM((8, 4, 4, 16, 512), F32),
            pltpu.VMEM((2, 6, 8, 32, 512), jnp.int16),
            pltpu.VMEM((2, 6, 8, 1, 512), F32),
            pltpu.VMEM((8, 4, 16, 512), F32),
            pltpu.VMEM((2, 3, 8, 16, 512), jnp.int16),
            pltpu.VMEM((2, 3, 8, 1, 512), F32),
            pltpu.VMEM((8, 16, 512), F32),
            dma((3,)),
            dma((1,)), dma((2, 4, 2)),
            dma((2, 2, 2)), dma((2, 2, 2)),
            dma((4,)), dma((4,)),
            dma((1,)), dma((2,)),
            dma((1,)), dma((2,)),
            dma((2,)), dma((2, 8)),
            dma((2,)), dma((2, 3, 8)),
            dma((2,)), dma((2, 8)),
            dma((1,)), dma((1,)),
        ],
        compiler_params=pltpu.CompilerParams(
            collective_id=0, has_side_effects=True, vmem_limit_bytes=60 * 1024 * 1024
        ),
        cost_estimate=pl.CostEstimate(flops=4_000_000_000, bytes_accessed=2_000_000, transcendentals=100_000),
        name="exchange",
    )(screened_blocks, density, basis_values, jnp.transpose(grid_points, (1, 0, 2)), grid_weights)
    return rows.reshape(128, 512).T.reshape(32, 16, 128)


def solution(mesh):
    placed = (
        P(None, "rows", "grid"),
        P("grid", None, "rows", None),
        P("grid", None, None),
        P("grid", None),
        P("grid", None),
    )
    return jax.shard_map(
        body, mesh=mesh, in_specs=placed, out_specs=P(None, "rows", "grid"), check_vma=False
    )
```

```python
import jax
import jax.numpy as jnp
from jax import lax
from jax.experimental import pallas as pl
from jax.experimental.pallas import tpu as pltpu
from jax.sharding import PartitionSpec as P

MESH = pl.DeviceIdType.MESH
NX = 4
NY = 4
NZ = 8
BF16 = jnp.bfloat16
F32 = jnp.float32
NT = (((1,), (1,)), ((), ()))
FAR_FIRST = (4, 3, 5, 2, 6, 1, 7)
LIMIT = 32767.0
TINY = 4.8e-38


def mod(a, n):
    return lax.rem(a, n)


def encode(values, codes, scales):
    largest = jnp.max(jnp.abs(values), axis=0, keepdims=True)
    parts = (values * 0.25) * (1.0 / (jnp.maximum(largest, TINY) * 0.25))
    codes[...] = jnp.round(parts * LIMIT).astype(jnp.int32).astype(jnp.int16)
    scales[...] = largest


def decode(codes, scales):
    return (codes[...].astype(jnp.int32).astype(F32) * (1.0 / LIMIT)) * scales[...]


def kernel(
    sel, dens, xin, pts, wts, out,
    inv, pg, xg, psel, tcol, scale, wcol, fs, fr, ps, pr, pot, xd, k0, k1, kp, kq, ks, s1, aq, az, t1, bq, bz, z1,
    o_s, x_s, x_r, p_s, p_r, q_s, q_r, f_s, f_r, m_s, m_r, d_s, d_r, a_s, a_r, b_s, b_r, z_s, z_r,
):
    g = lax.axis_index("grid")
    r = lax.axis_index("rows")
    core = mod(g, 2)
    chip = lax.div(g, 2)
    x = mod(chip, NX)
    y = lax.div(chip, NX)
    finish = []

    def at_plane(xx, yy):
        return (2 * (NX * yy + xx) + core, r)

    def at_z(rr):
        return (g, rr)

    partner = (2 * chip + 1 - core, r)
    up, down = at_z(mod(r + 1, NZ)), at_z(mod(r + NZ - 1, NZ))
    east, west = at_plane(mod(x + 1, NX), y), at_plane(mod(x + NX - 1, NX), y)
    north, south = at_plane(x, mod(y + 1, NY)), at_plane(x, mod(y + NY - 1, NY))

    def remote(src, dst, send, recv, device):
        return pltpu.make_async_remote_copy(
            src_ref=src, dst_ref=dst, send_sem=send, recv_sem=recv, device_id=device, device_id_type=MESH
        )

    own = [pltpu.make_async_copy(xin.at[b], xg.at[b, pl.ds(0, 16), r], o_s.at[b]) for b in range(2)]
    own.append(pltpu.make_async_copy(dens, pg.at[y, x, core], o_s.at[2]))
    for copy in own:
        copy.start()
    bar = pltpu.get_barrier_semaphore()
    for device in (up, down, east, west, north, south, partner):
        pl.semaphore_signal(bar, inc=1, device_id=device, device_id_type=MESH)
    pl.semaphore_wait(bar, 7)
    own[0].wait()

    def x_copy(d, t, b):
        shard = mod(r + (NZ - t if d == 0 else t), NZ)
        part = pl.ds(0, 16) if t < 3 else pl.ds(8 * d, 8)
        dst = xg.at[b, part, shard]
        return remote(dst, dst, x_s.at[0], x_r.at[d, t, b], up if d == 0 else down)

    def x_send(t, b):
        for d in range(2):
            if t > 0:
                x_copy(d, t - 1, b).wait_recv()
            x_copy(d, t, b).start()

    def px_copy(d, t):
        if t == 0:
            ref = pg.at[y, x, core]
        else:
            ref = pg.at[y, mod(x + (3 if d == 0 else 1), NX), core, pl.ds(16 * d, 16)]
        return remote(ref, ref, p_s.at[0, d, t], p_r.at[0, d, t], east if d == 0 else west)

    def py_copy(d, t):
        if t == 0:
            ref = pg.at[y, :, core]
        else:
            ref = pg.at[mod(y + (3 if d == 0 else 1), NY), :, core, pl.ds(16 * d, 16)]
        return remote(ref, ref, p_s.at[1, d, t], p_r.at[1, d, t], north if d == 0 else south)

    def pq_copy(k):
        ref = pg.at[mod(y + k, NY), :, core]
        return remote(ref, ref, q_s.at[k], q_r.at[k], partner)

    x_send(0, 0)
    own[2].wait()
    px_copy(0, 0).start()
    px_copy(1, 0).start()
    own[1].wait()
    x_send(0, 1)

    for rp in range(8):
        k0[rp, 16] = jnp.zeros(k0.shape[2:], F32)
    for half in range(2):
        k1[half, 16] = jnp.zeros(k1.shape[2:], F32)
    for b in range(2):
        xg[b, 16] = jnp.zeros(xg.shape[2:], BF16)

    px_copy(0, 0).wait_recv()
    px_copy(0, 1).start()
    px_copy(1, 0).wait_recv()
    px_copy(1, 1).start()

    @pl.loop(0, 32)
    def _(nb):
        for b in range(2):
            at = jnp.int32(16)
            for s in range(16):
                at = jnp.where(sel[b, s] == nb, s, at)
            inv[b, nb] = at

    x_send(1, 0)

    px_copy(0, 1).wait_recv()
    px_copy(1, 1).wait_recv()
    py_copy(0, 0).start()
    py_copy(1, 0).start()
    pq_copy(0).start()

    lanes = pl.ds(pl.multiple_of(128 * lax.div(r, 2), 128), 128)
    mine = pl.ds(pl.multiple_of(64 * mod(r, 2), 64), 64)
    for b in range(2):
        for c in range(4):
            row = pts[c, b : b + 1, lanes] if c < 3 else wts[b : b + 1, lanes]
            tcol[b, c] = jnp.broadcast_to(row, (128, 128)).T
        dist = jnp.zeros((64, 512), F32)
        for c in range(3):
            diff = pts[c, b : b + 1, :] - jnp.concatenate([tcol[b, c, mine]] * 4, axis=1)
            dist = dist + diff * diff
        scale[b] = wts[b : b + 1, :] * (1.0 / jnp.sqrt(dist + 0.5))
        wcol[b] = tcol[b, 3, mine]

    x_send(1, 1)
    x_send(2, 0)

    for d in range(2):
        py_copy(d, 0).wait_recv()
        py_copy(d, 1).start()
    pq_copy(1).start()
    pq_copy(3).start()

    x_send(2, 1)
    x_send(3, 0)

    py_copy(0, 1).wait_recv()
    py_copy(1, 1).wait_recv()
    pq_copy(2).start()

    x_send(3, 1)

    for k in range(4):
        pq_copy(k).wait_recv()

    def finish_gathers():
        sent = xg.at[:, pl.ds(0, 16), pl.ds(0, 7)]
        remote(sent, sent, x_s.at[0], x_r.at[0, 0, 0], up).wait_send()
        for d in range(2):
            for t in range(2):
                px_copy(d, t).wait_send()
                py_copy(d, t).wait_send()
        for k in range(4):
            pq_copy(k).wait_send()

    finish.append(finish_gathers)

    @pl.loop(0, 16)
    def _(s):
        for b in range(2):
            row = sel[b, s]
            for c in range(16):
                col = sel[b, c]
                psel[b, s, :, 128 * c : 128 * (c + 1)] = pg[
                    lax.div(col, 8), mod(lax.div(col, 2), 4), mod(col, 2), row
                ]

    def f_copy(b, k):
        to = mod(r + k, NZ)
        return remote(fs.at[b, to], fr.at[b, r], f_s.at[0], f_r.at[b], at_z(to))

    for b in range(2):
        for d in range(2):
            x_copy(d, 3, b).wait_recv()
        f = jnp.dot(
            psel[b].reshape(256, 2048), xg[b, 0:16].reshape(2048, 512), preferred_element_type=F32
        ).astype(BF16)
        fs[b] = f.T.reshape(8, 64, 256)
        for k in FAR_FIRST:
            f_copy(b, k).start()
        fr[b, r] = fs[b, r]

    def finish_f():
        some = pl.ds(0, 7)
        remote(fs.at[:, some], fr.at[:, some], f_s.at[0], f_r.at[0], up).wait_send()

    finish.append(finish_f)

    def m_copy(b, k):
        to = mod(r + k, NZ)
        return remote(ps.at[b, to], pr.at[b, r], m_s.at[0], m_r.at[b], at_z(to))

    for b in range(2):
        remote(fs.at[b, pl.ds(0, 7)], fr.at[b, pl.ds(0, 7)], f_s.at[0], f_r.at[b], up).wait_recv()
        inter = jnp.zeros((64, 512), F32)
        for s in range(8):
            inter = inter + jnp.dot(fr[b, s], xg[b, 0:16, s].reshape(256, 512), preferred_element_type=F32)
        mixed = (scale[b] * inter).astype(BF16)
        factor = jnp.concatenate([wcol[b]] * 2, axis=1)
        for s in range(8):
            p = lax.dot_general(mixed, xg[b, 0:16, s].reshape(256, 512), NT, preferred_element_type=F32)
            ps[b, s] = (p * factor).astype(BF16)
        for k in FAR_FIRST:
            m_copy(b, k).start()
        pr[b, r] = ps[b, r]

    def finish_m():
        some = pl.ds(0, 7)
        remote(ps.at[:, some], pr.at[:, some], m_s.at[0], m_r.at[0], up).wait_send()

    finish.append(finish_m)

    def potential(b):
        remote(ps.at[b, pl.ds(0, 7)], pr.at[b, pl.ds(0, 7)], m_s.at[0], m_r.at[b], up).wait_recv()
        pot[b] = pr[b].reshape(512, 256).T

    potential(0)

    @pl.loop(0, 8)
    def _(rp):
        for a in range(32):
            xd[8, a] = xg[0, inv[0, a], rp]
        k0[rp, 0:16] = lax.dot_general(
            pot[0], xd[8].reshape(512, 512), NT, preferred_element_type=F32
        ).reshape(16, 16, 512)
        for a in range(32):
            xd[rp, a] = xg[1, inv[1, a], rp]

    potential(1)

    first = (x, y)
    second = (y, x)

    def pair(codes, scales, code_sems, scale_sems, device):
        return (remote(*codes, *code_sems, device), remote(*scales, *scale_sems, device))

    def d_copy(rp):
        return pair(
            (kq.at[0, rp], kq.at[1, rp]), (ks.at[0, rp], ks.at[1, rp]),
            (d_s.at[0], d_r.at[0, rp]), (d_s.at[1], d_r.at[1, rp]), partner,
        )

    def start(copies):
        for copy in copies:
            copy.start()

    def wait_recv(copies):
        for copy in copies:
            copy.wait_recv()

    def wait_send(copies):
        for copy in copies:
            copy.wait_send()

    def along(half, stage, shift):
        if half == stage:
            return at_plane(mod(x + shift, NX), y)
        return at_plane(x, mod(y + shift, NY))

    def a_pair(rp, which, group, device):
        return pair(
            (aq.at[0, which, rp], aq.at[1, which, rp]), (az.at[0, which, rp], az.at[1, which, rp]),
            (a_s.at[0], a_r.at[0, group, rp]), (a_s.at[1], a_r.at[1, group, rp]), device,
        )

    def a_send(half, rp, m, values):
        encode(values.reshape(32, 512), aq.at[0, m, rp], az.at[0, m, rp])
        start(a_pair(rp, m, min(m, 2), along(half, 0, 1 if m % 2 == 0 else 3)))

    def a_value(rp, m):
        return decode(aq.at[1, m, rp], az.at[1, m, rp]).reshape(4, 8, 512)

    def b_pair(rp, which, device):
        return pair(
            (bq.at[0, which, rp], bq.at[1, which, rp]), (bz.at[0, which, rp], bz.at[1, which, rp]),
            (b_s.at[0], b_r.at[0, rp]), (b_s.at[1], b_r.at[1, rp]), device,
        )

    def make_slice(half, rp):
        k1[half, 0:16] = lax.dot_general(
            pot[1], xd[rp].reshape(512, 512), NT, preferred_element_type=F32
        ).reshape(16, 16, 512)
        for ref, c in ((kp, 1 - core), (s1, core)):
            for v in range(4):
                for u in range(4):
                    nb = 2 * (NX * v + u if half == 0 else NX * u + v) + c
                    ref[rp, v, u] = k0[rp, inv[0, nb]] + k1[half, inv[1, nb]]
            if ref is kp:
                for part in range(8):
                    encode(
                        kp[rp, part // 2, 2 * (part % 2) : 2 * (part % 2) + 2].reshape(32, 512),
                        kq.at[0, rp, pl.ds(32 * part, 32)], ks.at[0, rp, part],
                    )
                start(d_copy(rp))

    def send_slice(half, rp):
        wait_recv(d_copy(rp))
        for part in range(8):
            s1[rp, part // 2, 2 * (part % 2) : 2 * (part % 2) + 2] += decode(
                kq.at[1, rp, pl.ds(32 * part, 32)], ks.at[1, rp, part]
            ).reshape(2, 16, 512)
        u = first[half]
        a_send(half, rp, 0, s1[rp, :, mod(u + 2, 4), 0:8])
        a_send(half, rp, 1, s1[rp, :, mod(u + 2, 4), 8:16])
        a_send(half, rp, 2, s1[rp, :, mod(u + 1, 4), 8:16])
        a_send(half, rp, 3, s1[rp, :, mod(u + 3, 4), 0:8])

    def finish_a():
        def whole(codes, scales, send, recv):
            first_of = (0,) * (len(recv.shape) - 1)
            wait_send(
                pair(
                    (codes.at[0], codes.at[1]), (scales.at[0], scales.at[1]),
                    (send.at[0], recv.at[(0, *first_of)]), (send.at[1], recv.at[(1, *first_of)]), partner,
                )
            )

        whole(kq, ks, d_s, d_r)
        whole(aq, az, a_s, a_r)
        whole(bq, bz, b_s, b_r)

    finish.append(finish_a)

    def combine_slice(half, rp):
        u = first[half]
        wait_recv(a_pair(rp, 0, 0, partner))
        a_send(half, rp, 4, a_value(rp, 0) + s1[rp, :, mod(u + 1, 4), 0:8])
        wait_recv(a_pair(rp, 1, 1, partner))
        a_send(half, rp, 5, a_value(rp, 1) + s1[rp, :, mod(u + 3, 4), 8:16])

    def second_slice(half, rp):
        u = first[half]
        wait_recv(a_pair(rp, pl.ds(2, 4), 2, partner))
        t1[rp, :, 0:8] = s1[rp, :, u, 0:8] + a_value(rp, 3) + a_value(rp, 4)
        t1[rp, :, 8:16] = s1[rp, :, u, 8:16] + a_value(rp, 2) + a_value(rp, 5)
        for m in range(3):
            encode(t1[rp, mod(second[half] + (2, 1, 3)[m], 4)], bq.at[0, m, rp], bz.at[0, m, rp])
            start(b_pair(rp, m, along(half, 1, (2, 1, 3)[m])))

    def z_copy(rp):
        return remote(z1.at[rp], out.at[r], z_s.at[0], z_r.at[0], at_z(rp))

    def last_slice(half, rp):
        total = t1[rp, second[half]]
        wait_recv(b_pair(rp, pl.ds(0, 3), partner))
        for m in range(3):
            total = total + decode(bq.at[1, m, rp], bz.at[1, m, rp])
        z1[rp] = total

        @pl.when(rp != r)
        def _():
            z_copy(rp).start()

    plan = (
        (make_slice, 0), (make_slice, 1), (send_slice, 0), (make_slice, 2), (send_slice, 1), (make_slice, 3),
        (send_slice, 2), (combine_slice, 0), (send_slice, 3), (combine_slice, 1), (combine_slice, 2),
        (second_slice, 0), (combine_slice, 3), (second_slice, 1), (second_slice, 2), (last_slice, 0),
        (second_slice, 3), (last_slice, 1), (last_slice, 2), (last_slice, 3),
    )
    for stage, p in plan:
        stage(0, p)
        stage(1, p + 4)

    out[r] = z1[r]

    others = remote(z1.at[pl.ds(0, 7)], out.at[pl.ds(0, 7)], z_s.at[0], z_r.at[0], up)
    others.wait_recv()

    for waits in finish:
        waits()

    others.wait_send()


def body(density, basis_values, grid_points, grid_weights, screened_blocks):
    vmem = pl.BlockSpec(memory_space=pltpu.VMEM)
    hbm = pl.BlockSpec(memory_space=pl.ANY)
    smem = pl.BlockSpec(memory_space=pltpu.SMEM)
    dma = pltpu.SemaphoreType.DMA
    rows = pl.pallas_call(
        kernel,
        out_shape=jax.ShapeDtypeStruct((8, 16, 512), F32),
        in_specs=[smem, hbm, hbm, vmem, vmem],
        out_specs=vmem,
        scratch_shapes=[
            pltpu.SMEM((2, 32), jnp.int32),
            pltpu.VMEM((4, 4, 2, 32, 16, 128), BF16),
            pltpu.VMEM((2, 17, 8, 16, 512), BF16),
            pltpu.VMEM((2, 16, 16, 2048), BF16),
            pltpu.VMEM((2, 4, 128, 128), F32),
            pltpu.VMEM((2, 64, 512), F32),
            pltpu.VMEM((2, 64, 128), F32),
            pltpu.VMEM((2, 8, 64, 256), BF16),
            pltpu.VMEM((2, 8, 64, 256), BF16),
            pltpu.VMEM((2, 8, 64, 256), BF16),
            pltpu.VMEM((2, 8, 64, 256), BF16),
            pltpu.VMEM((2, 256, 512), BF16),
            pltpu.VMEM((9, 32, 16, 512), BF16),
            pltpu.VMEM((8, 17, 16, 512), F32),
            pltpu.VMEM((2, 17, 16, 512), F32),
            pltpu.VMEM((8, 4, 4, 16, 512), F32),
            pltpu.VMEM((2, 8, 256, 512), jnp.int16),
            pltpu.VMEM((2, 8, 8, 1, 512), F32),
            pltpu.VMEM((8, 4, 4, 16, 512), F32),
            pltpu.VMEM((2, 6, 8, 32, 512), jnp.int16),
            pltpu.VMEM((2, 6, 8, 1, 512), F32),
            pltpu.VMEM((8, 4, 16, 512), F32),
            pltpu.VMEM((2, 3, 8, 16, 512), jnp.int16),
            pltpu.VMEM((2, 3, 8, 1, 512), F32),
            pltpu.VMEM((8, 16, 512), F32),
            dma((3,)),
            dma((1,)), dma((2, 4, 2)),
            dma((2, 2, 2)), dma((2, 2, 2)),
            dma((4,)), dma((4,)),
            dma((1,)), dma((2,)),
            dma((1,)), dma((2,)),
            dma((2,)), dma((2, 8)),
            dma((2,)), dma((2, 3, 8)),
            dma((2,)), dma((2, 8)),
            dma((1,)), dma((1,)),
        ],
        compiler_params=pltpu.CompilerParams(
            collective_id=0, has_side_effects=True, vmem_limit_bytes=60 * 1024 * 1024
        ),
        cost_estimate=pl.CostEstimate(flops=4_000_000_000, bytes_accessed=2_000_000, transcendentals=100_000),
        name="exchange",
    )(screened_blocks, density, basis_values, jnp.transpose(grid_points, (1, 0, 2)), grid_weights)
    return rows.reshape(128, 512).T.reshape(32, 16, 128)


def solution(mesh):
    placed = (
        P(None, "rows", "grid"),
        P("grid", None, "rows", None),
        P("grid", None, None),
        P("grid", None),
        P("grid", None),
    )
    return jax.shard_map(
        body, mesh=mesh, in_specs=placed, out_specs=P(None, "rows", "grid"), check_vma=False
    )
```

```python
import jax
import jax.numpy as jnp
from jax import lax
from jax.experimental import pallas as pl
from jax.experimental.pallas import tpu as pltpu
from jax.sharding import PartitionSpec as P

MESH = pl.DeviceIdType.MESH
NX = 4
NY = 4
NZ = 8
BF16 = jnp.bfloat16
F32 = jnp.float32
NT = (((1,), (1,)), ((), ()))
FAR_FIRST = (4, 3, 5, 2, 6, 1, 7)
LIMIT = 32767.0
TINY = 4.8e-38


def mod(a, n):
    return lax.rem(a, n)


def encode(values, codes, scales):
    largest = jnp.max(jnp.abs(values), axis=0, keepdims=True)
    parts = (values * 0.25) * (1.0 / (jnp.maximum(largest, TINY) * 0.25))
    codes[...] = jnp.round(parts * LIMIT).astype(jnp.int32).astype(jnp.int16)
    scales[...] = largest


def decode(codes, scales):
    return (codes[...].astype(jnp.int32).astype(F32) * (1.0 / LIMIT)) * scales[...]


def kernel(
    sel, dens, xin, pts, wts, out,
    inv, pg, xg, psel, tcol, scale, wcol, fs, fr, ps, pr, pot, xd, k0, k1, kp, kq, ks, s1, aq, az, t1, bq, bz, z1,
    o_s, x_s, x_r, p_s, p_r, q_s, q_r, f_s, f_r, m_s, m_r, d_s, d_r, a_s, a_r, b_s, b_r, z_s, z_r,
):
    g = lax.axis_index("grid")
    r = lax.axis_index("rows")
    core = mod(g, 2)
    chip = lax.div(g, 2)
    x = mod(chip, NX)
    y = lax.div(chip, NX)
    finish = []

    def at_plane(xx, yy):
        return (2 * (NX * yy + xx) + core, r)

    def at_z(rr):
        return (g, rr)

    partner = (2 * chip + 1 - core, r)
    up, down = at_z(mod(r + 1, NZ)), at_z(mod(r + NZ - 1, NZ))
    east, west = at_plane(mod(x + 1, NX), y), at_plane(mod(x + NX - 1, NX), y)
    north, south = at_plane(x, mod(y + 1, NY)), at_plane(x, mod(y + NY - 1, NY))

    def remote(src, dst, send, recv, device):
        return pltpu.make_async_remote_copy(
            src_ref=src, dst_ref=dst, send_sem=send, recv_sem=recv, device_id=device, device_id_type=MESH
        )

    own = [pltpu.make_async_copy(xin.at[b], xg.at[b, pl.ds(0, 16), r], o_s.at[b]) for b in range(2)]
    own.append(pltpu.make_async_copy(dens, pg.at[y, x, core], o_s.at[2]))
    for copy in own:
        copy.start()
    bar = pltpu.get_barrier_semaphore()
    for device in (up, down, east, west, north, south, partner):
        pl.semaphore_signal(bar, inc=1, device_id=device, device_id_type=MESH)
    pl.semaphore_wait(bar, 7)
    own[0].wait()

    def x_copy(d, t, b):
        shard = mod(r + (NZ - t if d == 0 else t), NZ)
        part = pl.ds(0, 16) if t < 3 else pl.ds(8 * d, 8)
        dst = xg.at[b, part, shard]
        return remote(dst, dst, x_s.at[0], x_r.at[d, t, b], up if d == 0 else down)

    def x_send(t, b):
        for d in range(2):
            if t > 0:
                x_copy(d, t - 1, b).wait_recv()
            x_copy(d, t, b).start()

    def px_copy(d, t):
        if t == 0:
            ref = pg.at[y, x, core]
        else:
            ref = pg.at[y, mod(x + (3 if d == 0 else 1), NX), core, pl.ds(16 * d, 16)]
        return remote(ref, ref, p_s.at[0], p_r.at[0, d, t], east if d == 0 else west)

    def py_copy(d, t):
        if t == 0:
            ref = pg.at[y, :, core]
        else:
            ref = pg.at[mod(y + (3 if d == 0 else 1), NY), :, core, pl.ds(16 * d, 16)]
        return remote(ref, ref, p_s.at[1], p_r.at[1, d, t], north if d == 0 else south)

    def pq_copy(k):
        ref = pg.at[mod(y + k, NY), :, core]
        return remote(ref, ref, q_s.at[0], q_r.at[0], partner)

    x_send(0, 0)
    own[2].wait()
    px_copy(0, 0).start()
    px_copy(1, 0).start()
    own[1].wait()
    x_send(0, 1)

    for rp in range(8):
        k0[rp, 16] = jnp.zeros(k0.shape[2:], F32)
    for half in range(2):
        k1[half, 16] = jnp.zeros(k1.shape[2:], F32)
    for b in range(2):
        xg[b, 16] = jnp.zeros(xg.shape[2:], BF16)

    px_copy(0, 0).wait_recv()
    px_copy(0, 1).start()
    px_copy(1, 0).wait_recv()
    px_copy(1, 1).start()

    @pl.loop(0, 32)
    def _(nb):
        for b in range(2):
            at = jnp.int32(16)
            for s in range(16):
                at = jnp.where(sel[b, s] == nb, s, at)
            inv[b, nb] = at

    x_send(1, 0)

    px_copy(0, 1).wait_recv()
    px_copy(1, 1).wait_recv()
    py_copy(0, 0).start()
    py_copy(1, 0).start()
    pq_copy(0).start()

    lanes = pl.ds(pl.multiple_of(128 * lax.div(r, 2), 128), 128)
    mine = pl.ds(pl.multiple_of(64 * mod(r, 2), 64), 64)
    for b in range(2):
        for c in range(4):
            row = pts[c, b : b + 1, lanes] if c < 3 else wts[b : b + 1, lanes]
            tcol[b, c] = jnp.broadcast_to(row, (128, 128)).T
        dist = jnp.zeros((64, 512), F32)
        for c in range(3):
            diff = pts[c, b : b + 1, :] - jnp.concatenate([tcol[b, c, mine]] * 4, axis=1)
            dist = dist + diff * diff
        scale[b] = wts[b : b + 1, :] * (1.0 / jnp.sqrt(dist + 0.5))
        wcol[b] = tcol[b, 3, mine]

    x_send(1, 1)
    x_send(2, 0)

    for d in range(2):
        py_copy(d, 0).wait_recv()
        py_copy(d, 1).start()
    pq_copy(1).start()
    pq_copy(3).start()

    x_send(2, 1)
    x_send(3, 0)

    py_copy(0, 1).wait_recv()
    py_copy(1, 1).wait_recv()
    pq_copy(2).start()

    x_send(3, 1)

    half_grid = pg.at[:, :, core]
    to_partner = remote(half_grid, pg.at[:, :, 1 - core], q_s.at[0], q_r.at[0], partner)
    to_partner.wait_recv()

    def finish_gathers():
        sent = xg.at[:, pl.ds(0, 16), pl.ds(0, 7)]
        remote(sent, sent, x_s.at[0], x_r.at[0, 0, 0], up).wait_send()
        line, plane = pg.at[0, pl.ds(0, 3), core], pg.at[pl.ds(0, 3), :, core]
        remote(line, line, p_s.at[0], p_r.at[0, 0, 0], east).wait_send()
        remote(plane, plane, p_s.at[1], p_r.at[1, 0, 0], north).wait_send()
        to_partner.wait_send()

    finish.append(finish_gathers)

    @pl.loop(0, 16)
    def _(s):
        for b in range(2):
            row = sel[b, s]
            for c in range(16):
                col = sel[b, c]
                psel[b, s, :, 128 * c : 128 * (c + 1)] = pg[
                    lax.div(col, 8), mod(lax.div(col, 2), 4), mod(col, 2), row
                ]

    def f_copy(b, k):
        to = mod(r + k, NZ)
        return remote(fs.at[b, to], fr.at[b, r], f_s.at[0], f_r.at[b], at_z(to))

    for b in range(2):
        for d in range(2):
            x_copy(d, 3, b).wait_recv()
        f = jnp.dot(
            psel[b].reshape(256, 2048), xg[b, 0:16].reshape(2048, 512), preferred_element_type=F32
        ).astype(BF16)
        fs[b] = f.T.reshape(8, 64, 256)
        for k in FAR_FIRST:
            f_copy(b, k).start()
        fr[b, r] = fs[b, r]

    def finish_f():
        some = pl.ds(0, 7)
        remote(fs.at[:, some], fr.at[:, some], f_s.at[0], f_r.at[0], up).wait_send()

    finish.append(finish_f)

    def m_copy(b, k):
        to = mod(r + k, NZ)
        return remote(ps.at[b, to], pr.at[b, r], m_s.at[0], m_r.at[b], at_z(to))

    for b in range(2):
        remote(fs.at[b, pl.ds(0, 7)], fr.at[b, pl.ds(0, 7)], f_s.at[0], f_r.at[b], up).wait_recv()
        inter = jnp.zeros((64, 512), F32)
        for s in range(8):
            inter = inter + jnp.dot(fr[b, s], xg[b, 0:16, s].reshape(256, 512), preferred_element_type=F32)
        mixed = (scale[b] * inter).astype(BF16)
        factor = jnp.concatenate([wcol[b]] * 2, axis=1)
        for s in range(8):
            p = lax.dot_general(mixed, xg[b, 0:16, s].reshape(256, 512), NT, preferred_element_type=F32)
            ps[b, s] = (p * factor).astype(BF16)
        for k in FAR_FIRST:
            m_copy(b, k).start()
        pr[b, r] = ps[b, r]

    def finish_m():
        some = pl.ds(0, 7)
        remote(ps.at[:, some], pr.at[:, some], m_s.at[0], m_r.at[0], up).wait_send()

    finish.append(finish_m)

    def potential(b):
        remote(ps.at[b, pl.ds(0, 7)], pr.at[b, pl.ds(0, 7)], m_s.at[0], m_r.at[b], up).wait_recv()
        pot[b] = pr[b].reshape(512, 256).T

    potential(0)

    @pl.loop(0, 8)
    def _(rp):
        for a in range(32):
            xd[8, a] = xg[0, inv[0, a], rp]
        k0[rp, 0:16] = lax.dot_general(
            pot[0], xd[8].reshape(512, 512), NT, preferred_element_type=F32
        ).reshape(16, 16, 512)
        for a in range(32):
            xd[rp, a] = xg[1, inv[1, a], rp]

    potential(1)

    first = (x, y)
    second = (y, x)

    def pair(codes, scales, code_sems, scale_sems, device):
        return (remote(*codes, *code_sems, device), remote(*scales, *scale_sems, device))

    def d_copy(rp):
        return pair(
            (kq.at[0, rp], kq.at[1, rp]), (ks.at[0, rp], ks.at[1, rp]),
            (d_s.at[0], d_r.at[0, rp]), (d_s.at[1], d_r.at[1, rp]), partner,
        )

    def start(copies):
        for copy in copies:
            copy.start()

    def wait_recv(copies):
        for copy in copies:
            copy.wait_recv()

    def wait_send(copies):
        for copy in copies:
            copy.wait_send()

    def along(half, stage, shift):
        if half == stage:
            return at_plane(mod(x + shift, NX), y)
        return at_plane(x, mod(y + shift, NY))

    def a_pair(rp, which, group, device):
        return pair(
            (aq.at[0, which, rp], aq.at[1, which, rp]), (az.at[0, which, rp], az.at[1, which, rp]),
            (a_s.at[0], a_r.at[0, group, rp]), (a_s.at[1], a_r.at[1, group, rp]), device,
        )

    def a_send(half, rp, m, values):
        encode(values.reshape(32, 512), aq.at[0, m, rp], az.at[0, m, rp])
        start(a_pair(rp, m, m // 2 if m < 2 else 1, along(half, 0, 1 if m % 2 == 0 else 3)))

    def a_value(rp, m):
        return decode(aq.at[1, m, rp], az.at[1, m, rp]).reshape(4, 8, 512)

    def b_pair(rp, which, device):
        return pair(
            (bq.at[0, which, rp], bq.at[1, which, rp]), (bz.at[0, which, rp], bz.at[1, which, rp]),
            (b_s.at[0], b_r.at[0, rp]), (b_s.at[1], b_r.at[1, rp]), device,
        )

    def make_slice(half, rp):
        k1[half, 0:16] = lax.dot_general(
            pot[1], xd[rp].reshape(512, 512), NT, preferred_element_type=F32
        ).reshape(16, 16, 512)
        for ref, c in ((kp, 1 - core), (s1, core)):
            for v in range(4):
                for u in range(4):
                    nb = 2 * (NX * v + u if half == 0 else NX * u + v) + c
                    ref[rp, v, u] = k0[rp, inv[0, nb]] + k1[half, inv[1, nb]]
            if ref is kp:
                for part in range(8):
                    encode(
                        kp[rp, part // 2, 2 * (part % 2) : 2 * (part % 2) + 2].reshape(32, 512),
                        kq.at[0, rp, pl.ds(32 * part, 32)], ks.at[0, rp, part],
                    )
                start(d_copy(rp))

    def send_slice(half, rp):
        wait_recv(d_copy(rp))
        for part in range(8):
            s1[rp, part // 2, 2 * (part % 2) : 2 * (part % 2) + 2] += decode(
                kq.at[1, rp, pl.ds(32 * part, 32)], ks.at[1, rp, part]
            ).reshape(2, 16, 512)
        u = first[half]
        a_send(half, rp, 0, s1[rp, :, mod(u + 2, 4), 0:8])
        a_send(half, rp, 1, s1[rp, :, mod(u + 2, 4), 8:16])
        a_send(half, rp, 2, s1[rp, :, mod(u + 1, 4), 8:16])
        a_send(half, rp, 3, s1[rp, :, mod(u + 3, 4), 0:8])

    def finish_a():
        def whole(codes, scales, send, recv):
            first_of = (0,) * (len(recv.shape) - 1)
            wait_send(
                pair(
                    (codes.at[0], codes.at[1]), (scales.at[0], scales.at[1]),
                    (send.at[0], recv.at[(0, *first_of)]), (send.at[1], recv.at[(1, *first_of)]), partner,
                )
            )

        whole(kq, ks, d_s, d_r)
        whole(aq, az, a_s, a_r)
        whole(bq, bz, b_s, b_r)

    finish.append(finish_a)

    def combine_slice(half, rp):
        u = first[half]
        wait_recv(a_pair(rp, pl.ds(0, 2), 0, partner))
        a_send(half, rp, 4, a_value(rp, 0) + s1[rp, :, mod(u + 1, 4), 0:8])
        a_send(half, rp, 5, a_value(rp, 1) + s1[rp, :, mod(u + 3, 4), 8:16])

    def second_slice(half, rp):
        u = first[half]
        wait_recv(a_pair(rp, pl.ds(2, 4), 1, partner))
        t1[rp, :, 0:8] = s1[rp, :, u, 0:8] + a_value(rp, 3) + a_value(rp, 4)
        t1[rp, :, 8:16] = s1[rp, :, u, 8:16] + a_value(rp, 2) + a_value(rp, 5)
        for m in range(3):
            encode(t1[rp, mod(second[half] + (2, 1, 3)[m], 4)], bq.at[0, m, rp], bz.at[0, m, rp])
            start(b_pair(rp, m, along(half, 1, (2, 1, 3)[m])))

    def z_copy(rp):
        return remote(z1.at[rp], out.at[r], z_s.at[0], z_r.at[0], at_z(rp))

    def last_slice(half, rp):
        total = t1[rp, second[half]]
        wait_recv(b_pair(rp, pl.ds(0, 3), partner))
        for m in range(3):
            total = total + decode(bq.at[1, m, rp], bz.at[1, m, rp])
        z1[rp] = total

        @pl.when(rp != r)
        def _():
            z_copy(rp).start()

    plan = (
        (make_slice, 0), (make_slice, 1), (send_slice, 0), (make_slice, 2), (send_slice, 1), (make_slice, 3),
        (send_slice, 2), (combine_slice, 0), (send_slice, 3), (combine_slice, 1), (combine_slice, 2),
        (second_slice, 0), (combine_slice, 3), (second_slice, 1), (second_slice, 2), (last_slice, 0),
        (second_slice, 3), (last_slice, 1), (last_slice, 2), (last_slice, 3),
    )
    for stage, p in plan:
        stage(0, p)
        stage(1, p + 4)

    out[r] = z1[r]

    others = remote(z1.at[pl.ds(0, 7)], out.at[pl.ds(0, 7)], z_s.at[0], z_r.at[0], up)
    others.wait_recv()

    for waits in finish:
        waits()

    others.wait_send()


def body(density, basis_values, grid_points, grid_weights, screened_blocks):
    vmem = pl.BlockSpec(memory_space=pltpu.VMEM)
    hbm = pl.BlockSpec(memory_space=pl.ANY)
    smem = pl.BlockSpec(memory_space=pltpu.SMEM)
    dma = pltpu.SemaphoreType.DMA
    rows = pl.pallas_call(
        kernel,
        out_shape=jax.ShapeDtypeStruct((8, 16, 512), F32),
        in_specs=[smem, hbm, hbm, vmem, vmem],
        out_specs=vmem,
        scratch_shapes=[
            pltpu.SMEM((2, 32), jnp.int32),
            pltpu.VMEM((4, 4, 2, 32, 16, 128), BF16),
            pltpu.VMEM((2, 17, 8, 16, 512), BF16),
            pltpu.VMEM((2, 16, 16, 2048), BF16),
            pltpu.VMEM((2, 4, 128, 128), F32),
            pltpu.VMEM((2, 64, 512), F32),
            pltpu.VMEM((2, 64, 128), F32),
            pltpu.VMEM((2, 8, 64, 256), BF16),
            pltpu.VMEM((2, 8, 64, 256), BF16),
            pltpu.VMEM((2, 8, 64, 256), BF16),
            pltpu.VMEM((2, 8, 64, 256), BF16),
            pltpu.VMEM((2, 256, 512), BF16),
            pltpu.VMEM((9, 32, 16, 512), BF16),
            pltpu.VMEM((8, 17, 16, 512), F32),
            pltpu.VMEM((2, 17, 16, 512), F32),
            pltpu.VMEM((8, 4, 4, 16, 512), F32),
            pltpu.VMEM((2, 8, 256, 512), jnp.int16),
            pltpu.VMEM((2, 8, 8, 1, 512), F32),
            pltpu.VMEM((8, 4, 4, 16, 512), F32),
            pltpu.VMEM((2, 6, 8, 32, 512), jnp.int16),
            pltpu.VMEM((2, 6, 8, 1, 512), F32),
            pltpu.VMEM((8, 4, 16, 512), F32),
            pltpu.VMEM((2, 3, 8, 16, 512), jnp.int16),
            pltpu.VMEM((2, 3, 8, 1, 512), F32),
            pltpu.VMEM((8, 16, 512), F32),
            dma((3,)),
            dma((1,)), dma((2, 4, 2)),
            dma((2,)), dma((2, 2, 2)),
            dma((1,)), dma((1,)),
            dma((1,)), dma((2,)),
            dma((1,)), dma((2,)),
            dma((2,)), dma((2, 8)),
            dma((2,)), dma((2, 2, 8)),
            dma((2,)), dma((2, 8)),
            dma((1,)), dma((1,)),
        ],
        compiler_params=pltpu.CompilerParams(
            collective_id=0, has_side_effects=True, vmem_limit_bytes=60 * 1024 * 1024
        ),
        cost_estimate=pl.CostEstimate(flops=4_000_000_000, bytes_accessed=2_000_000, transcendentals=100_000),
        name="exchange",
    )(screened_blocks, density, basis_values, jnp.transpose(grid_points, (1, 0, 2)), grid_weights)
    return rows.reshape(128, 512).T.reshape(32, 16, 128)


def solution(mesh):
    placed = (
        P(None, "rows", "grid"),
        P("grid", None, "rows", None),
        P("grid", None, None),
        P("grid", None),
        P("grid", None),
    )
    return jax.shard_map(
        body, mesh=mesh, in_specs=placed, out_specs=P(None, "rows", "grid"), check_vma=False
    )
```
